256 devices in a mesh: grp: 2 (over z), scen: 128 (over x, y, core).
Axes of the slice: x: 8, y: 8, z: 2, core: 2. Of those that a mesh axis runs over, the one named last changes fastest.
The devices are a block of a 8x8x16 slice.
Arguments:
- shocks: bfloat16 [262144, 2048], P(('grp', 'scen')), parts along dimension 0, may hold values from -8 to 8
- factor_sens: bfloat16 [2048, 1024], replicated, may hold values from -0.13258252 to 0.13258252
- notional: float32 [1024], replicated, may hold values from -0.25 to 0.25
- moneyness: float32 [1024], replicated, may hold values from -2 to 2
- desk_entity: int32 [64], replicated, may hold values from 0 to 7
- scenario_counts: int32 [256], P(('grp', 'scen')), parts along dimension 0, may hold values from 256 to 1024, as said below
- candidate_ids: int32 [2048], P('grp'), parts along dimension 0, may hold values from 0 to 131071, as said below
Outputs:
- tail_losses: float32 [512], P('grp'), parts along dimension 0
- cand_entity: float32 [2048, 8], P(('grp', 'scen')), parts along dimension 0
The draws below stay inside these ranges and needn't reach their ends.
There are 2 independent parts, one for each index of `grp`. The reference program is written for one: setup_inputs(seed, part) draws one part's arguments, and reference() takes and returns one part's arrays. A program takes and returns all parts, laid end to end along the dimension named above; an argument that names none is the same for every part. Nothing has to cross between parts.
Inputs may be any that keep to these rules, and one draw needn't show every extreme that they name: `scenario_counts`: every block has at least 256 valid scenarios; some block in every draw is full. `candidate_ids`: each id b * 1024 + j names a valid scenario: j is below scenario_counts[b].
All inputs are finite; a program needn't handle non-finite values.
Results may differ from the reference program's by a relative error of at most 0.0003.
Values sent between devices are 32-bit elements; how exact they have to be, the bound alone decides.
A program may use at most 128 MiB of HBM per device.

```python
import jax
import jax.numpy as jnp
from jax import lax

F = 2048
K = 64
INSTR = 16
ENT = 8
TOPK = 256
CAND = 1024
S_DEV = 1024
N_SCEN = 128


def common_draw(key):
    base = jax.random.fold_in(key, 7)
    key_a, key_b, key_c, key_d = jax.random.split(base, 4)
    counts = jax.random.randint(key_a, (N_SCEN,), S_DEV // 4, S_DEV + 1)
    filled = jax.random.randint(key_b, (), 0, N_SCEN)
    counts = jnp.where(jnp.arange(N_SCEN) == filled, S_DEV, counts).astype(jnp.int32)
    owners = jax.random.randint(key_c, (CAND,), 0, N_SCEN)
    offsets = jax.random.randint(key_d, (CAND,), 0, counts[owners])
    return (counts, (owners * S_DEV + offsets).astype(jnp.int32), filled)


def draw_scenario_counts(key, part):
    return common_draw(key)[0]


def draw_candidate_ids(key, part):
    return common_draw(key)[1]


def draw_shocks(key, part):
    filled = common_draw(key)[2]
    noise_key = jax.random.fold_in(key, 11)
    moves = jax.random.normal(noise_key, (S_DEV * N_SCEN, F), jnp.float32)
    hot_scale = 2.0
    block_of_row = jnp.arange(S_DEV * N_SCEN, dtype=jnp.int32) // S_DEV
    scales = jnp.where(block_of_row == filled, jnp.float32(hot_scale), jnp.float32(1.0))
    return jnp.clip(moves * scales[:, None], -8.0, 8.0).astype(jnp.bfloat16)


def draw_factor_sens(key, part):
    half = K * INSTR // 2
    key_a, key_b = jax.random.split(jax.random.fold_in(key, 21))
    first = jnp.clip(jax.random.normal(key_a, (F, half), jnp.float32), -4.0, 4.0)
    second = jnp.clip(jax.random.normal(key_b, (F, half), jnp.float32), -4.0, 4.0)
    paired = jnp.stack([first, -first + 0.15 * second], axis=2).reshape(F, K * INSTR)
    return (paired * F ** (-0.5)).astype(jnp.bfloat16)


def draw_notional(key, part):
    half = K * INSTR // 2
    scale = 2.0 * (K * INSTR) ** (-0.5)
    noise_key = jax.random.fold_in(key, 31)
    values = jnp.clip(jax.random.normal(noise_key, (half,), jnp.float32), -4.0, 4.0)
    return jnp.repeat(values * scale, 2).astype(jnp.float32)


def draw_moneyness(key, part):
    half = K * INSTR // 2
    noise_key = jax.random.fold_in(key, 41)
    values = jax.random.uniform(noise_key, (half,), jnp.float32, -2.0, 2.0)
    return jnp.repeat(values, 2).astype(jnp.float32)


def set_ends(entries, stream_key, least, top_value):
    longest = entries.shape.index(max(entries.shape))
    spots = []
    for shift in (0, 1):
        where = [jax.random.randint(jax.random.fold_in(stream_key, axis), (), 0, length) for axis, length in enumerate(entries.shape)]
        where[longest] = (where[longest] + shift) % entries.shape[longest]
        spots.append(tuple(where))
    return entries.at[spots[0]].set(least).at[spots[1]].set(top_value)


def setup_inputs(seed: int = 0, part: int = 0) -> dict:
    arg_keys = jax.random.split(jax.random.key(seed), 8)
    part_keys = jax.random.split(jax.random.fold_in(arg_keys[7], part), 8)
    shocks = draw_shocks(jax.random.fold_in(jax.random.fold_in(arg_keys[7], part), 71), part)
    factor_sens = draw_factor_sens(jax.random.fold_in(arg_keys[7], 71), part)
    notional = draw_notional(jax.random.fold_in(arg_keys[7], 71), part)
    moneyness = draw_moneyness(jax.random.fold_in(arg_keys[7], 71), part)
    desk_entity = set_ends(jax.random.randint(arg_keys[4], (K,), 0, ENT), jax.random.fold_in(arg_keys[4], 1), 0, ENT - 1).astype(jnp.int32)
    scenario_counts = draw_scenario_counts(jax.random.fold_in(jax.random.fold_in(arg_keys[7], part), 71), part)
    candidate_ids = draw_candidate_ids(jax.random.fold_in(jax.random.fold_in(arg_keys[7], part), 71), part)
    return {"shocks": shocks, "factor_sens": factor_sens, "notional": notional, "moneyness": moneyness, "desk_entity": desk_entity, "scenario_counts": scenario_counts, "candidate_ids": candidate_ids}


def price(rows, factor_sens, notional, moneyness):
    value = jnp.dot(rows, factor_sens, preferred_element_type=jnp.float32)
    inst = notional * (jax.nn.softplus(value + moneyness) - jax.nn.softplus(moneyness))
    return jnp.sum(inst.reshape(rows.shape[0], K, INSTR), axis=2)


def reference(shocks, factor_sens, notional, moneyness, desk_entity, scenario_counts, candidate_ids):
    blocks = shocks.reshape(N_SCEN, S_DEV, F)

    def one_block(item):
        rows, count = item
        loss = -jnp.sum(price(rows, factor_sens, notional, moneyness), axis=1)
        valid = jnp.arange(S_DEV, dtype=jnp.int32) < count
        return jnp.where(valid, loss, jnp.float32(-1e30))

    losses = lax.map(one_block, (blocks, scenario_counts))
    tail_losses = lax.top_k(losses.reshape(-1), TOPK)[0]
    cand_rows = jnp.take(shocks, candidate_ids, axis=0)
    cand_pnl = price(cand_rows, factor_sens, notional, moneyness)
    onehot = (desk_entity[:, None] == jnp.arange(ENT, dtype=jnp.int32)[None, :]).astype(jnp.float32)
    cand_entity = -jnp.dot(cand_pnl, onehot, precision=lax.Precision.HIGHEST)
    return tail_losses, cand_entity
```

```python
import functools

import jax
import jax.numpy as jnp
from jax import lax
from jax.experimental import pallas as pl
from jax.experimental.pallas import tpu as pltpu
from jax.sharding import PartitionSpec as P

K = 64
INSTR = 16
ENT = 8
TOPK = 256
SIDE = 8
CORES = 2
LANES = 128
SUB = 8
TILE = 256
FLOOR = -1e30
MESH = pl.DeviceIdType.MESH
F32 = jnp.float32
BF16 = jnp.bfloat16


def iota(shape, dim):
    return lax.broadcasted_iota(jnp.int32, shape, dim)


def pieces(array, count):
    out = []
    for _ in range(count):
        part = array.astype(BF16).astype(F32)
        out.append(part)
        array = array - part
    return out


def pair_sum(left, right, step):
    low = (iota(left.shape, 1) & step) == 0
    up = left + pltpu.roll(left, LANES - step, 1)
    down = right + pltpu.roll(right, step, 1)
    return jnp.where(low, up, down)


def merge(stored, own, step, after):
    value = stored * own
    x = jnp.maximum(value, pltpu.roll(value, step, 1)) * after
    for stride in (128, 64, 32, 16, 8):
        y = x.reshape(TOPK // (2 * stride), 2, stride, LANES)
        a, b = y[:, 0], y[:, 1]
        x = jnp.stack([jnp.maximum(a, b), jnp.minimum(a, b)], axis=1).reshape(TOPK, LANES)
    y = x.reshape(TOPK // SUB, SUB, LANES)
    at = iota(y.shape, 1)
    for stride in (4, 2, 1):
        low = (at & stride) == 0
        if stride == 4:
            other = pltpu.roll(y, 4, 1)
        else:
            other = jnp.where(low, pltpu.roll(y, SUB - stride, 1), pltpu.roll(y, stride, 1))
        y = jnp.where(low, jnp.maximum(y, other), jnp.minimum(y, other))
    return y.reshape(TOPK, LANES)


def lists_down(rows):
    copies = LANES // rows.shape[0]
    return jnp.concatenate([rows] * copies, axis=0).T


def along_lanes(column):
    same = iota(column.shape, 0) == iota(column.shape, 1)
    return jnp.sum(jnp.where(same, column, 0.0), axis=0, keepdims=True)


def sign_of(bit):
    return jnp.where(bit, F32(-1.0), F32(1.0))


def kernel(
    shocks, sens, notional, moneyness, desk_entity, counts, ids,
    tail_out, cand_out,
    sh, fs, nv, mv, dv, cv, iv, indicator, column, spread, gathered,
    list1, list2, got1, got2, cand1, cand2, cgot1, cgot2, flipped,
    load_sem, small_sem, send1, recv1, send2, recv2, csend1, crecv1, csend2, crecv2,
):
    slots = sh.shape[0]
    turns = slots // TILE
    chunks = sens.shape[1] // TILE
    me = lax.axis_index("scen")
    x, yc = me // (SIDE * CORES), me % (SIDE * CORES)
    half = SIDE * CORES
    across = [lax.rem(x + d, SIDE) for d in range(1, SIDE)]
    along = [lax.rem(yc + d, half) for d in range(1, half)]

    def load_rows(r):
        rows = pl.ds(r * TILE, TILE)
        return pltpu.make_async_copy(shocks.at[rows], sh.at[rows], load_sem.at[r])

    def load_columns(c):
        cols = pl.ds(c * TILE, TILE)
        return pltpu.make_async_copy(sens.at[:, cols], fs.at[:, cols], load_sem.at[turns + c])

    small = [
        pltpu.make_async_copy(src, dst, small_sem.at[n])
        for n, (src, dst) in enumerate(
            [(moneyness, mv), (notional, nv), (desk_entity, dv), (counts, cv), (ids, iv)]
        )
    ]
    load_rows(0).start()
    load_columns(0).start()
    for copy in small:
        copy.start()
    for c in range(1, chunks):
        load_columns(c).start()
    for r in range(1, turns):
        load_rows(r).start()

    barrier = pltpu.get_barrier_semaphore()
    for other in across:
        pl.semaphore_signal(barrier, inc=1, device_id={"scen": other * half + yc}, device_id_type=MESH)
    for other in along:
        pl.semaphore_signal(barrier, inc=1, device_id={"scen": x * half + other}, device_id_type=MESH)

    for copy in small:
        copy.wait()

    lane = iota((TILE, LANES), 0)
    within = lane % LANES
    desk = 8 * (4 * (lane // LANES) + 2 * ((within // 4) % 2) + (within // 8) % 2) + within // 16
    place = jnp.where(desk == iota((TILE, LANES), 1), 1.0, 0.0).astype(BF16)
    entity = jnp.concatenate([dv[...], jnp.full((1, LANES - K), -1, jnp.int32)], axis=1)
    row = iota((TILE, LANES), 0)
    member = jnp.where(row < ENT, row, jnp.where(row >= LANES, -2, -3))
    hit = (entity == member) | ((member == -2) & (iota((TILE, LANES), 1) < K))
    owner = jnp.where(hit, -1.0, 0.0).astype(BF16)
    indicator[...] = lax.dot_general(
        place, owner, (((1,), (1,)), ((), ())), preferred_element_type=F32
    ).astype(BF16)
    gathered[...] = jnp.zeros(gathered.shape, F32)
    base = me * slots
    count = cv[0]

    def turn(r, first):
        load_rows(r).wait()
        rows = sh[pl.ds(r * TILE, TILE), :]
        sums = []
        for c in range(chunks):
            if first:
                load_columns(c).wait()
            value = jnp.dot(rows, fs[:, c * TILE:(c + 1) * TILE], preferred_element_type=F32)
            halves = []
            for h in range(2):
                b = 2 * c + h
                m = mv[b:b + 1, :]
                start = jnp.maximum(m, 0.0) + jnp.log(1.0 + jnp.exp(-jnp.abs(m)))
                v = value[:, h * LANES:(h + 1) * LANES] + m
                soft = jnp.maximum(v, 0.0) + jnp.log(1.0 + jnp.exp(-jnp.abs(v)))
                halves.append(nv[b:b + 1, :] * (soft - start))
            sums.append(pair_sum(halves[0], halves[1], 8))
        parts = jnp.concatenate(
            [pair_sum(sums[0], sums[1], 4), pair_sum(sums[2], sums[3], 4)], axis=1
        )
        total = jnp.zeros((TILE, TILE), F32)
        for part in pieces(parts, 3):
            total += jnp.dot(part.astype(BF16), indicator[...], preferred_element_type=F32)
        here = r * TILE + iota((TILE, LANES), 0)
        loss = jnp.where(here < count, total[:, LANES:], FLOOR)
        column[pl.ds(r * TILE, TILE), :] = loss
        for h in range(2):
            spread[2 * r + h] = loss[h * LANES:(h + 1) * LANES].T[0:SUB]
        by_entity = total[:, :LANES].T[0:ENT]
        left = jnp.concatenate(pieces(by_entity, 3), axis=0).astype(BF16)
        wanted = jnp.concatenate(
            [
                jnp.where(iv[b:b + 1, :] - base == here, 1.0, 0.0).astype(BF16)
                for b in range(SIDE)
            ],
            axis=1,
        )
        gathered[...] += jnp.dot(left, wanted, preferred_element_type=F32)

    turn(0, True)

    @pl.loop(1, turns)
    def _(r):
        turn(r, False)

    blocks = slots // LANES
    groups = slots // SUB
    level = []
    for i in range(blocks):
        mine = column[i * LANES:(i + 1) * LANES, :].reshape(LANES // SUB, SUB, LANES)
        seen = jnp.zeros(mine.shape, F32)
        for b in range(blocks):
            theirs = spread[b][None]
            if b < i:
                ahead = theirs >= mine
            elif b > i:
                ahead = theirs > mine
            else:
                own = iota(mine.shape, 0) * SUB + iota(mine.shape, 1)
                ahead = (theirs > mine) | ((theirs == mine) & (iota(mine.shape, 2) < own))
            seen = jnp.where(ahead, seen + 1.0, seen)
        level.append(seen.reshape(LANES, LANES))
    seen = jnp.concatenate(level, axis=0).astype(BF16)
    rank = jnp.dot(seen, jnp.ones((LANES, LANES), BF16), preferred_element_type=F32)

    rising1 = x >= SIDE // 2
    sign1 = sign_of(rising1)
    local = []
    for h in range(2):
        target = iota((1, LANES), 1).astype(F32) + float(h * LANES)
        target = jnp.where(rising1, float(TOPK - 1) - target, target)
        local.append(jnp.sum(jnp.where(rank == target, column[...], 0.0), axis=0, keepdims=True) * sign1)
    for h in range(2):
        list1[0, h:h + 1, :] = local[h]
    merged = gathered[...]
    total = merged[0:ENT] + merged[ENT:2 * ENT] + merged[2 * ENT:3 * ENT]
    for b in range(SIDE):
        cand1[b] = total[:, b * LANES:(b + 1) * LANES]

    pl.semaphore_wait(barrier, SIDE - 1 + half - 1)

    def to(src, dst, ssem, rsem, device):
        return pltpu.make_async_remote_copy(
            src_ref=src, dst_ref=dst, send_sem=ssem, recv_sem=rsem,
            device_id={"scen": device}, device_id_type=MESH,
        )

    first = [to(list1.at[0], got1.at[x], send1.at[o], recv1.at[x], o * half + yc) for o in across]
    cfirst = [to(cand1.at[o], cgot1.at[x], csend1.at[o], crecv1.at[x], o * half + yc) for o in across]
    for copy in first:
        copy.start()
    for copy in cfirst:
        copy.start()
    got1[x] = list1[0]
    cgot1[x] = cand1[x]

    def landed(dst, sem):
        pltpu.make_async_copy(dst, dst, sem).wait()

    for o in across:
        landed(got1.at[o], recv1.at[o])
    slot = iota((1, LANES), 1)
    all1 = got1[...]
    lists = jnp.concatenate([lists_down(all1[:, h, :]) for h in range(2)], axis=0)
    rising2 = yc >= half // 2
    lists = merge(lists, sign_of((slot & 4) != 0), 4, sign_of((slot & 2) != 0))
    lists = merge(lists, sign_of((slot & 2) != 0), 2, sign_of((slot & 1) != 0))
    lists = merge(lists, sign_of((slot & 1) != 0), 1, sign_of(rising2))
    for h in range(2):
        list2[0, h:h + 1, :] = along_lanes(lists[h * LANES:(h + 1) * LANES])
    second = [to(list2.at[0], got2.at[yc], send2.at[o], recv2.at[yc], x * half + o) for o in along]
    for copy in second:
        copy.start()
    got2[yc] = list2[0]

    for o in across:
        landed(cgot1.at[o], crecv1.at[o])
    cand2[0] = jnp.sum(cgot1[...], axis=0)
    csecond = [to(cand2.at[0], cgot2.at[yc], csend2.at[o], crecv2.at[yc], x * half + o) for o in along]
    for copy in csecond:
        copy.start()
    cgot2[yc] = cand2[0]

    for o in along:
        landed(got2.at[o], recv2.at[o])
    all2 = got2[...]
    lists = jnp.concatenate([lists_down(all2[:, h, :]) for h in range(2)], axis=0)
    lists = merge(lists, sign_of((slot & 8) != 0), 8, sign_of((slot & 4) != 0))
    lists = merge(lists, sign_of((slot & 4) != 0), 4, sign_of((slot & 2) != 0))
    lists = merge(lists, sign_of((slot & 2) != 0), 2, sign_of((slot & 1) != 0))
    lists = merge(lists, sign_of((slot & 1) != 0), 1, F32(1.0))
    for h in range(2):
        tail_out[h:h + 1, :] = along_lanes(lists[h * LANES:(h + 1) * LANES])

    for o in along:
        landed(cgot2.at[o], crecv2.at[o])
    summed = jnp.sum(cgot2[...], axis=0)
    flipped[...] = jnp.concatenate([summed] * (LANES // ENT), axis=0).T
    cand_out[...] = flipped[pl.ds(pl.multiple_of(yc * SUB, SUB), SUB), 0:ENT]

    for copy in first + cfirst + second + csecond:
        copy.wait_send()


def body(shocks, factor_sens, notional, moneyness, desk_entity, scenario_counts, candidate_ids):
    slots, factors = shocks.shape
    instruments = factor_sens.shape[1]
    half = SIDE * CORES
    any_space = pl.BlockSpec(memory_space=pl.ANY)
    vmem = pl.BlockSpec(memory_space=pltpu.VMEM)
    dma = pltpu.SemaphoreType.DMA
    tail, cand = pl.pallas_call(
        kernel,
        out_shape=(
            jax.ShapeDtypeStruct((2, LANES), F32),
            jax.ShapeDtypeStruct((SUB, ENT), F32),
        ),
        in_specs=[any_space] * 7,
        out_specs=(vmem, vmem),
        scratch_shapes=[
            pltpu.VMEM((slots, factors), BF16),
            pltpu.VMEM((factors, instruments), BF16),
            pltpu.VMEM((SUB, LANES), F32),
            pltpu.VMEM((SUB, LANES), F32),
            pltpu.VMEM((1, K), jnp.int32),
            pltpu.SMEM((1,), jnp.int32),
            pltpu.VMEM((SUB, LANES), jnp.int32),
            pltpu.VMEM((TILE, TILE), BF16),
            pltpu.VMEM((slots, LANES), F32),
            pltpu.VMEM((slots // LANES, SUB, LANES), F32),
            pltpu.VMEM((3 * ENT, SIDE * LANES), F32),
            pltpu.VMEM((1, 2, LANES), F32),
            pltpu.VMEM((1, 2, LANES), F32),
            pltpu.VMEM((SIDE, 2, LANES), F32),
            pltpu.VMEM((half, 2, LANES), F32),
            pltpu.VMEM((SIDE, ENT, LANES), F32),
            pltpu.VMEM((1, ENT, LANES), F32),
            pltpu.VMEM((SIDE, ENT, LANES), F32),
            pltpu.VMEM((half, ENT, LANES), F32),
            pltpu.VMEM((LANES, LANES), F32),
            dma((slots // TILE + instruments // TILE,)),
            dma((5,)),
            dma((SIDE,)), dma((SIDE,)), dma((half,)), dma((half,)),
            dma((SIDE,)), dma((SIDE,)), dma((half,)), dma((half,)),
        ],
        compiler_params=pltpu.CompilerParams(
            collective_id=0, has_side_effects=True, vmem_limit_bytes=48 * 1024 * 1024
        ),
        name="tail_search",
    )(
        shocks,
        factor_sens,
        notional.reshape(SUB, LANES),
        moneyness.reshape(SUB, LANES),
        desk_entity.reshape(1, K),
        scenario_counts,
        candidate_ids.reshape(SUB, LANES),
    )
    return tail.reshape(TOPK), cand


def solution(mesh):
    both = ("grp", "scen")
    return jax.shard_map(
        body,
        mesh=mesh,
        in_specs=(P(both, None), P(), P(), P(), P(), P(both), P("grp")),
        out_specs=(P("grp"), P(both, None)),
        check_vma=False,
    )
```

```python
import functools

import jax
import jax.numpy as jnp
from jax import lax
from jax.experimental import pallas as pl
from jax.experimental.pallas import tpu as pltpu
from jax.sharding import PartitionSpec as P

K = 64
INSTR = 16
ENT = 8
TOPK = 256
SIDE = 8
CORES = 2
LANES = 128
SUB = 8
TILE = 256
STRIP = 32
PIECES = 3
FAR_SIDE = (4, 3, 5, 2, 6, 1, 7)
FAR_HALF = (8, 9, 7, 6, 10, 5, 11, 4, 12, 3, 13, 2, 14, 1, 15)
FLOOR = -1e30
MESH = pl.DeviceIdType.MESH
F32 = jnp.float32
BF16 = jnp.bfloat16


def iota(shape, dim):
    return lax.broadcasted_iota(jnp.int32, shape, dim)


def pieces(array, count):
    out = []
    for _ in range(count):
        part = array.astype(BF16).astype(F32)
        out.append(part)
        array = array - part
    return out


def pair_sum(left, right, step):
    low = (iota(left.shape, 1) & step) == 0
    up = left + pltpu.roll(left, LANES - step, 1)
    down = right + pltpu.roll(right, step, 1)
    return jnp.where(low, up, down)


def merge(stored, own, step, after):
    value = stored * own
    x = jnp.maximum(value, pltpu.roll(value, step, 1)) * after
    for stride in (128, 64, 32, 16, 8):
        y = x.reshape(TOPK // (2 * stride), 2, stride, LANES)
        a, b = y[:, 0], y[:, 1]
        x = jnp.stack([jnp.maximum(a, b), jnp.minimum(a, b)], axis=1).reshape(TOPK, LANES)
    y = x.reshape(TOPK // SUB, SUB, LANES)
    at = iota(y.shape, 1)
    for stride in (4, 2, 1):
        low = (at & stride) == 0
        if stride == 4:
            other = pltpu.roll(y, 4, 1)
        else:
            other = jnp.where(low, pltpu.roll(y, SUB - stride, 1), pltpu.roll(y, stride, 1))
        y = jnp.where(low, jnp.maximum(y, other), jnp.minimum(y, other))
    return y.reshape(TOPK, LANES)


def lists_down(rows):
    copies = LANES // rows.shape[0]
    return jnp.concatenate([rows] * copies, axis=0).T


def along_lanes(column):
    same = iota(column.shape, 0) == iota(column.shape, 1)
    return jnp.sum(jnp.where(same, column, 0.0), axis=0, keepdims=True)


def sign_of(bit):
    return jnp.where(bit, F32(-1.0), F32(1.0))


def kernel(
    shocks, sens, notional, moneyness, desk_entity, counts, ids,
    tail_out, cand_out,
    sh, fs, nv, mv, dv, cv, iv, value, base_soft, terms, indicator, column, spread, seen, gathered,
    list1, list2, got1, got2, cand1, cand2, cgot1, cgot2, flipped,
    load_sem, small_sem, send1, recv1, send2, recv2, csend1, crecv1, csend2, crecv2,
):
    slots, factors = sh.shape
    turns = slots // TILE
    wide = sens.shape[1] // 2
    deep = factors // 2
    me = lax.axis_index("scen")
    x, yc = me // (SIDE * CORES), me % (SIDE * CORES)
    half = SIDE * CORES
    across = [lax.rem(x + d, SIDE) for d in FAR_SIDE]
    along = [lax.rem(yc + d, half) for d in FAR_HALF]

    def copy_in(src, dst, n):
        return pltpu.make_async_copy(src, dst, load_sem.at[n])

    def part(ref, r0, rn, c0, cn):
        return ref.at[pl.ds(r0, rn), pl.ds(c0, cn)]

    def load(n, r=None):
        if n == "rows":
            rows = pl.ds(r * TILE, TILE)
            return copy_in(shocks.at[rows], sh.at[rows], 4 + r)
        if n == "right":
            return copy_in(part(sens, 0, factors, wide, wide), part(fs, 0, factors, wide, wide), 4)
        k = n % 2
        if n < 2:
            where = (0, TILE, k * deep, deep)
            return copy_in(part(shocks, *where), part(sh, *where), n)
        where = (k * deep, deep, 0, wide)
        return copy_in(part(sens, *where), part(fs, *where), n)

    small = [
        pltpu.make_async_copy(src, dst, small_sem.at[n])
        for n, (src, dst) in enumerate(
            [(moneyness, mv), (notional, nv), (desk_entity, dv), (counts, cv), (ids, iv)]
        )
    ]
    for n in (0, 2, 1, 3):
        load(n).start()
    for copy in small:
        copy.start()
    for r in range(1, turns):
        load("rows", r).start()
    load("right").start()

    barrier = pltpu.get_barrier_semaphore()
    for other in across:
        pl.semaphore_signal(barrier, inc=1, device_id={"scen": other * half + yc}, device_id_type=MESH)
    for other in along:
        pl.semaphore_signal(barrier, inc=1, device_id={"scen": x * half + other}, device_id_type=MESH)

    for copy in small:
        copy.wait()

    lane = iota((TILE, LANES), 0)
    within = lane % LANES
    desk = 8 * (4 * (lane // LANES) + 2 * ((within // 4) % 2) + (within // 8) % 2) + within // 16
    place = jnp.where(desk == iota((TILE, LANES), 1), 1.0, 0.0).astype(BF16)
    entity = jnp.concatenate([dv[...], jnp.full((1, LANES - K), -1, jnp.int32)], axis=1)
    row = iota((TILE, LANES), 0)
    member = jnp.where(row < ENT, row, jnp.where(row >= LANES, -2, -3))
    hit = (entity == member) | ((member == -2) & (iota((TILE, LANES), 1) < K))
    owner = jnp.where(hit, -1.0, 0.0).astype(BF16)
    owner = lax.dot_general(
        place, owner, (((1,), (1,)), ((), ())), preferred_element_type=F32
    ).astype(BF16)
    for p in range(PIECES):
        indicator[p * TILE:(p + 1) * TILE, :] = owner
    money = mv[...]
    base_soft[...] = jnp.maximum(money, 0.0) + jnp.log(1.0 + jnp.exp(-jnp.abs(money)))
    gathered[...] = jnp.zeros(gathered.shape, F32)
    base = me * slots
    count = cv[0]

    def price(r, c):
        for s in range(0, TILE, STRIP):
            quads = []
            for h in range(4):
                b = 4 * c + h
                v = value[s:s + STRIP, h * LANES:(h + 1) * LANES] + mv[b:b + 1, :]
                soft = jnp.maximum(v, 0.0) + jnp.log(1.0 + jnp.exp(-jnp.abs(v)))
                quads.append(nv[b:b + 1, :] * (soft - base_soft[b:b + 1, :]))
            sums = pair_sum(
                pair_sum(quads[0], quads[1], 8), pair_sum(quads[2], quads[3], 8), 4
            )
            for p, term in enumerate(pieces(sums, PIECES)):
                at = p * TILE + c * LANES
                terms[pl.ds(r * TILE + s, STRIP), at:at + LANES] = term.astype(BF16)

    def multiply(r, c):
        value[...] = jnp.dot(
            sh[pl.ds(r * TILE, TILE), :], fs[:, c * wide:(c + 1) * wide], preferred_element_type=F32
        )

    def finish(r):
        rows = slice(r * TILE, (r + 1) * TILE)
        total = jnp.dot(terms[rows, :], indicator[...], preferred_element_type=F32)
        here = r * TILE + iota((TILE, LANES), 0)
        loss = jnp.where(here < count, total[:, LANES:], FLOOR)
        column[rows, :] = loss
        for h in range(2):
            spread[2 * r + h] = loss[h * LANES:(h + 1) * LANES].T[0:SUB]
        by_entity = total[:, :LANES].T[0:ENT]
        left = jnp.concatenate(pieces(by_entity, 3), axis=0).astype(BF16)
        wanted = jnp.concatenate(
            [
                jnp.where(iv[b:b + 1, :] - base == here, 1.0, 0.0).astype(BF16)
                for b in range(SIDE)
            ],
            axis=1,
        )
        gathered[...] += jnp.dot(left, wanted, preferred_element_type=F32)

    def compare(i, bs, fresh):
        rows = slice(i * LANES, (i + 1) * LANES)
        mine = column[rows, :].reshape(LANES // SUB, SUB, LANES)
        if fresh:
            before = jnp.zeros(mine.shape, F32)
        else:
            before = seen[rows, :].reshape(mine.shape)
        for b in bs:
            theirs = spread[b][None]
            if b < i:
                ahead = theirs >= mine
            elif b > i:
                ahead = theirs > mine
            else:
                own = iota(mine.shape, 0) * SUB + iota(mine.shape, 1)
                ahead = (theirs > mine) | ((theirs == mine) & (iota(mine.shape, 2) < own))
            before = jnp.where(ahead, before + 1.0, before)
        seen[rows, :] = before.reshape(LANES, LANES)

    def rank(r):
        for i in range(2 * r):
            compare(i, (2 * r, 2 * r + 1), False)
        for i in (2 * r, 2 * r + 1):
            compare(i, range(2 * r + 2), True)

    load(0).wait()
    load(2).wait()
    value[...] = jnp.dot(sh[0:TILE, 0:deep], fs[0:deep, 0:wide], preferred_element_type=F32)
    load(1).wait()
    load(3).wait()
    value[...] += jnp.dot(sh[0:TILE, deep:], fs[deep:, 0:wide], preferred_element_type=F32)

    @pl.loop(1, turns)
    def _(r):
        load("rows", r).wait()
        price(r - 1, 0)
        multiply(r, 0)

    load("right").wait()
    price(turns - 1, 0)
    multiply(0, 1)
    for r in range(turns):
        if r > 1:
            rank(r - 2)
        if r > 0:
            finish(r - 1)
        price(r, 1)
        if r < turns - 1:
            multiply(r + 1, 1)
    rank(turns - 2)
    finish(turns - 1)
    rank(turns - 1)

    rising1 = x >= SIDE // 2
    sign1 = sign_of(rising1)
    targets = []
    for h in range(2):
        target = iota((1, LANES), 1).astype(F32) + float(h * LANES)
        targets.append(jnp.where(rising1, float(TOPK - 1) - target, target))
    local = [jnp.zeros((SUB, LANES), F32) for _ in range(2)]
    for i in range(slots // LANES):
        rows = slice(i * LANES, (i + 1) * LANES)
        place = jnp.sum(seen[rows, :], axis=1, keepdims=True)
        for h in range(2):
            chosen = jnp.where(place == targets[h], column[rows, :], 0.0)
            local[h] += jnp.sum(chosen.reshape(LANES // SUB, SUB, LANES), axis=0)
    for h in range(2):
        list1[0, h:h + 1, :] = jnp.sum(local[h], axis=0, keepdims=True) * sign1
    merged = gathered[...]
    total = merged[0:ENT] + merged[ENT:2 * ENT] + merged[2 * ENT:3 * ENT]
    for b in range(SIDE):
        cand1[b] = total[:, b * LANES:(b + 1) * LANES]

    pl.semaphore_wait(barrier, SIDE - 1 + half - 1)

    def to(src, dst, ssem, rsem, device):
        return pltpu.make_async_remote_copy(
            src_ref=src, dst_ref=dst, send_sem=ssem, recv_sem=rsem,
            device_id={"scen": device}, device_id_type=MESH,
        )

    first = [to(list1.at[0], got1.at[x], send1.at[o], recv1.at[x], o * half + yc) for o in across]
    cfirst = [to(cand1.at[o], cgot1.at[x], csend1.at[o], crecv1.at[x], o * half + yc) for o in across]
    for copy in first:
        copy.start()
    for copy in cfirst:
        copy.start()
    got1[x] = list1[0]
    cgot1[x] = cand1[x]

    def landed(dst, sem):
        pltpu.make_async_copy(dst, dst, sem).wait()

    for o in across:
        landed(got1.at[o], recv1.at[o])
    slot = iota((1, LANES), 1)
    all1 = got1[...]
    lists = jnp.concatenate([lists_down(all1[:, h, :]) for h in range(2)], axis=0)
    rising2 = yc >= half // 2
    lists = merge(lists, sign_of((slot & 4) != 0), 4, sign_of((slot & 2) != 0))
    lists = merge(lists, sign_of((slot & 2) != 0), 2, sign_of((slot & 1) != 0))
    lists = merge(lists, sign_of((slot & 1) != 0), 1, sign_of(rising2))
    for h in range(2):
        list2[0, h:h + 1, :] = along_lanes(lists[h * LANES:(h + 1) * LANES])
    second = [to(list2.at[0], got2.at[yc], send2.at[o], recv2.at[yc], x * half + o) for o in along]
    for copy in second:
        copy.start()
    got2[yc] = list2[0]

    for o in across:
        landed(cgot1.at[o], crecv1.at[o])
    cand2[0] = jnp.sum(cgot1[...], axis=0)
    csecond = [to(cand2.at[0], cgot2.at[yc], csend2.at[o], crecv2.at[yc], x * half + o) for o in along]
    for copy in csecond:
        copy.start()
    cgot2[yc] = cand2[0]

    for o in along:
        landed(got2.at[o], recv2.at[o])
    all2 = got2[...]
    lists = jnp.concatenate([lists_down(all2[:, h, :]) for h in range(2)], axis=0)
    lists = merge(lists, sign_of((slot & 8) != 0), 8, sign_of((slot & 4) != 0))
    lists = merge(lists, sign_of((slot & 4) != 0), 4, sign_of((slot & 2) != 0))
    lists = merge(lists, sign_of((slot & 2) != 0), 2, sign_of((slot & 1) != 0))
    lists = merge(lists, sign_of((slot & 1) != 0), 1, F32(1.0))
    for h in range(2):
        tail_out[h:h + 1, :] = along_lanes(lists[h * LANES:(h + 1) * LANES])

    for o in along:
        landed(cgot2.at[o], crecv2.at[o])
    summed = jnp.sum(cgot2[...], axis=0)
    flipped[...] = jnp.concatenate([summed] * (LANES // ENT), axis=0).T
    cand_out[...] = flipped[pl.ds(pl.multiple_of(yc * SUB, SUB), SUB), 0:ENT]

    for copy in first + cfirst + second + csecond:
        copy.wait_send()


def body(shocks, factor_sens, notional, moneyness, desk_entity, scenario_counts, candidate_ids):
    slots, factors = shocks.shape
    instruments = factor_sens.shape[1]
    half = SIDE * CORES
    hbm = pl.BlockSpec(memory_space=pltpu.HBM)
    vmem = pl.BlockSpec(memory_space=pltpu.VMEM)
    dma = pltpu.SemaphoreType.DMA
    tail, cand = pl.pallas_call(
        kernel,
        out_shape=(
            jax.ShapeDtypeStruct((2, LANES), F32),
            jax.ShapeDtypeStruct((SUB, ENT), F32),
        ),
        in_specs=[hbm] * 7,
        out_specs=(vmem, vmem),
        scratch_shapes=[
            pltpu.VMEM((slots, factors), BF16),
            pltpu.VMEM((factors, instruments), BF16),
            pltpu.VMEM((SUB, LANES), F32),
            pltpu.VMEM((SUB, LANES), F32),
            pltpu.VMEM((1, K), jnp.int32),
            pltpu.SMEM((1,), jnp.int32),
            pltpu.VMEM((SUB, LANES), jnp.int32),
            pltpu.VMEM((TILE, instruments // 2), F32),
            pltpu.VMEM((SUB, LANES), F32),
            pltpu.VMEM((slots, PIECES * TILE), BF16),
            pltpu.VMEM((PIECES * TILE, TILE), BF16),
            pltpu.VMEM((slots, LANES), F32),
            pltpu.VMEM((slots // LANES, SUB, LANES), F32),
            pltpu.VMEM((slots, LANES), F32),
            pltpu.VMEM((3 * ENT, SIDE * LANES), F32),
            pltpu.VMEM((1, 2, LANES), F32),
            pltpu.VMEM((1, 2, LANES), F32),
            pltpu.VMEM((SIDE, 2, LANES), F32),
            pltpu.VMEM((half, 2, LANES), F32),
            pltpu.VMEM((SIDE, ENT, LANES), F32),
            pltpu.VMEM((1, ENT, LANES), F32),
            pltpu.VMEM((SIDE, ENT, LANES), F32),
            pltpu.VMEM((half, ENT, LANES), F32),
            pltpu.VMEM((LANES, LANES), F32),
            dma((4 + slots // TILE,)),
            dma((5,)),
            dma((SIDE,)), dma((SIDE,)), dma((half,)), dma((half,)),
            dma((SIDE,)), dma((SIDE,)), dma((half,)), dma((half,)),
        ],
        compiler_params=pltpu.CompilerParams(
            collective_id=0, has_side_effects=True, vmem_limit_bytes=67043328
        ),
        name="tail_search",
    )(
        shocks,
        factor_sens,
        notional.reshape(SUB, LANES),
        moneyness.reshape(SUB, LANES),
        desk_entity.reshape(1, K),
        scenario_counts,
        candidate_ids.reshape(SUB, LANES),
    )
    return tail.reshape(TOPK), cand


def solution(mesh):
    both = ("grp", "scen")
    return jax.shard_map(
        body,
        mesh=mesh,
        in_specs=(P(both, None), P(), P(), P(), P(), P(both), P("grp")),
        out_specs=(P("grp"), P(both, None)),
        check_vma=False,
    )
```

```python
import functools

import jax
import jax.numpy as jnp
from jax import lax
from jax.experimental import pallas as pl
from jax.experimental.pallas import tpu as pltpu
from jax.sharding import PartitionSpec as P

K = 64
INSTR = 16
ENT = 8
TOPK = 256
SIDE = 8
CORES = 2
LANES = 128
SUB = 8
TILE = 256
STRIP = 32
PIECES = 3
FAR_SIDE = (4, 3, 5, 2, 6, 1, 7)
FAR_HALF = (8, 9, 7, 6, 10, 5, 11, 4, 12, 3, 13, 2, 14, 1, 15)
FLOOR = -1e30
MESH = pl.DeviceIdType.MESH
F32 = jnp.float32
BF16 = jnp.bfloat16


def iota(shape, dim):
    return lax.broadcasted_iota(jnp.int32, shape, dim)


def pieces(array, count):
    out = []
    for _ in range(count):
        part = array.astype(BF16).astype(F32)
        out.append(part)
        array = array - part
    return out


def pair_sum(left, right, step):
    low = (iota(left.shape, 1) & step) == 0
    up = left + pltpu.roll(left, LANES - step, 1)
    down = right + pltpu.roll(right, step, 1)
    return jnp.where(low, up, down)


def merge(stored, own, step, after):
    value = stored * own
    x = jnp.maximum(value, pltpu.roll(value, step, 1)) * after
    for stride in (128, 64, 32, 16, 8):
        y = x.reshape(TOPK // (2 * stride), 2, stride, LANES)
        a, b = y[:, 0], y[:, 1]
        x = jnp.stack([jnp.maximum(a, b), jnp.minimum(a, b)], axis=1).reshape(TOPK, LANES)
    y = x.reshape(TOPK // SUB, SUB, LANES)
    at = iota(y.shape, 1)
    for stride in (4, 2, 1):
        low = (at & stride) == 0
        if stride == 4:
            other = pltpu.roll(y, 4, 1)
        else:
            other = jnp.where(low, pltpu.roll(y, SUB - stride, 1), pltpu.roll(y, stride, 1))
        y = jnp.where(low, jnp.maximum(y, other), jnp.minimum(y, other))
    return y.reshape(TOPK, LANES)


def lists_down(rows):
    copies = LANES // rows.shape[0]
    return jnp.concatenate([rows] * copies, axis=0).T


def along_lanes(column):
    same = iota(column.shape, 0) == iota(column.shape, 1)
    return jnp.sum(jnp.where(same, column, 0.0), axis=0, keepdims=True)


def sign_of(bit):
    return jnp.where(bit, F32(-1.0), F32(1.0))


def kernel(
    cv, shocks, sens, notional, moneyness, desk_entity, ids,
    tail_out, cand_out,
    sh, fs, nv, mv, dv, iv, value, base_soft, terms, indicator, column, spread, seen, gathered,
    list1, list2, got1, got2, cand1, cand2, cgot1, cgot2, flipped,
    load_sem, small_sem, send1, recv1, send2, recv2, csend1, crecv1, csend2, crecv2,
):
    slots, factors = sh.shape
    turns = slots // TILE
    wide = sens.shape[1] // 2
    deep = factors // 2
    me = lax.axis_index("scen")
    x, yc = me // (SIDE * CORES), me % (SIDE * CORES)
    half = SIDE * CORES
    across = [lax.rem(x + d, SIDE) for d in FAR_SIDE]
    along = [lax.rem(yc + d, half) for d in FAR_HALF]

    def copy_in(src, dst, n):
        return pltpu.make_async_copy(src, dst, load_sem.at[n])

    def part(ref, r0, rn, c0, cn):
        return ref.at[pl.ds(r0, rn), pl.ds(c0, cn)]

    def load(n, r=None):
        if n == "rows":
            rows = pl.ds(r * TILE, TILE)
            return copy_in(shocks.at[rows], sh.at[rows], 4 + r)
        if n == "right":
            return copy_in(part(sens, 0, factors, wide, wide), part(fs, 0, factors, wide, wide), 4)
        k = n % 2
        if n < 2:
            where = (0, TILE, k * deep, deep)
            return copy_in(part(shocks, *where), part(sh, *where), n)
        where = (k * deep, deep, 0, wide)
        return copy_in(part(sens, *where), part(fs, *where), n)

    small = [
        pltpu.make_async_copy(src, dst, small_sem.at[n])
        for n, (src, dst) in enumerate(
            [(moneyness, mv), (notional, nv), (desk_entity, dv), (ids, iv)]
        )
    ]
    for n in (0, 2, 1, 3):
        load(n).start()
    for copy in small:
        copy.start()
    for r in range(1, turns):
        load("rows", r).start()
    load("right").start()

    barrier = pltpu.get_barrier_semaphore()
    for other in across:
        pl.semaphore_signal(barrier, inc=1, device_id={"scen": other * half + yc}, device_id_type=MESH)
    for other in along:
        pl.semaphore_signal(barrier, inc=1, device_id={"scen": x * half + other}, device_id_type=MESH)

    for copy in small:
        copy.wait()

    lane = iota((LANES, LANES), 0)
    desk = 8 * (4 * ((lane // 2) % 2) + 2 * ((lane // 4) % 2) + (lane // 8) % 2) + lane // 16
    place = jnp.where(desk == iota((LANES, LANES), 1), 1.0, 0.0).astype(BF16)
    entity = jnp.concatenate([dv[...], jnp.full((1, LANES - K), -1, jnp.int32)], axis=1)
    row = iota((TILE, LANES), 0)
    member = jnp.where(row < ENT, row, jnp.where(row >= LANES, -2, -3))
    hit = (entity == member) | ((member == -2) & (iota((TILE, LANES), 1) < K))
    owner = jnp.where(hit, -1.0, 0.0).astype(BF16)
    owner = lax.dot_general(
        place, owner, (((1,), (1,)), ((), ())), preferred_element_type=F32
    ).astype(BF16)
    for p in range(PIECES):
        indicator[p * LANES:(p + 1) * LANES, :] = owner
    money = mv[...]
    base_soft[...] = jnp.maximum(money, 0.0) + jnp.log(1.0 + jnp.exp(-jnp.abs(money)))
    gathered[...] = jnp.zeros(gathered.shape, F32)
    base = me * slots
    count = cv[0]

    def price(r, c):
        for s in range(0, TILE, STRIP):
            quads = []
            for h in range(4):
                b = 4 * c + h
                v = value[s:s + STRIP, h * LANES:(h + 1) * LANES] + mv[b:b + 1, :]
                soft = jnp.maximum(v, 0.0) + jnp.log(1.0 + jnp.exp(-jnp.abs(v)))
                quads.append(nv[b:b + 1, :] * (soft - base_soft[b:b + 1, :]))
            sums = pair_sum(
                pair_sum(quads[0], quads[1], 8), pair_sum(quads[2], quads[3], 8), 4
            )
            rows = pl.ds(r * TILE + s, STRIP)
            if c == 0:
                column[rows, :] = sums
            else:
                sums = pair_sum(column[rows, :], sums, 2)
                for p, term in enumerate(pieces(sums, PIECES)):
                    terms[rows, p * LANES:(p + 1) * LANES] = term.astype(BF16)

    def multiply(r, c):
        value[...] = jnp.dot(
            sh[pl.ds(r * TILE, TILE), :], fs[:, c * wide:(c + 1) * wide], preferred_element_type=F32
        )

    def finish(r):
        rows = slice(r * TILE, (r + 1) * TILE)
        total = jnp.concatenate(
            [
                jnp.dot(
                    terms[r * TILE + h * LANES:r * TILE + (h + 1) * LANES, :], indicator[...],
                    preferred_element_type=F32,
                )
                for h in range(2)
            ],
            axis=0,
        )
        here = r * TILE + iota((TILE, LANES), 0)
        loss = jnp.where(here < count, total[:, LANES:], FLOOR)
        column[rows, :] = loss
        for h in range(2):
            spread[2 * r + h] = loss[h * LANES:(h + 1) * LANES].T[0:SUB]
        by_entity = total[:, :LANES].T[0:ENT]
        left = jnp.concatenate(pieces(by_entity, 3), axis=0).astype(BF16)
        wanted = jnp.concatenate(
            [
                jnp.where(iv[b:b + 1, :] - base == here, 1.0, 0.0).astype(BF16)
                for b in range(SIDE)
            ],
            axis=1,
        )
        gathered[...] += jnp.dot(left, wanted, preferred_element_type=F32)

    def compare(i, bs, fresh):
        rows = slice(i * LANES, (i + 1) * LANES)
        mine = column[rows, :].reshape(LANES // SUB, SUB, LANES)
        if fresh:
            before = jnp.zeros(mine.shape, F32)
        else:
            before = seen[rows, :].reshape(mine.shape)
        for b in bs:
            theirs = spread[b][None]
            if b < i:
                ahead = theirs >= mine
            elif b > i:
                ahead = theirs > mine
            else:
                own = iota(mine.shape, 0) * SUB + iota(mine.shape, 1)
                ahead = (theirs > mine) | ((theirs == mine) & (iota(mine.shape, 2) < own))
            before = jnp.where(ahead, before + 1.0, before)
        seen[rows, :] = before.reshape(LANES, LANES)

    def rank(r):
        for i in range(2 * r):
            compare(i, (2 * r, 2 * r + 1), False)
        for i in (2 * r, 2 * r + 1):
            compare(i, range(2 * r + 2), True)

    load(0).wait()
    load(2).wait()
    value[...] = jnp.dot(sh[0:TILE, 0:deep], fs[0:deep, 0:wide], preferred_element_type=F32)
    load(1).wait()
    load(3).wait()
    value[...] += jnp.dot(sh[0:TILE, deep:], fs[deep:, 0:wide], preferred_element_type=F32)

    @pl.loop(1, turns)
    def _(r):
        load("rows", r).wait()
        price(r - 1, 0)
        multiply(r, 0)

    load("right").wait()
    price(turns - 1, 0)
    multiply(0, 1)
    for r in range(turns):
        if r > 1:
            rank(r - 2)
        if r > 0:
            finish(r - 1)
        price(r, 1)
        if r < turns - 1:
            multiply(r + 1, 1)
    rank(turns - 2)
    finish(turns - 1)
    rank(turns - 1)

    rising1 = x >= SIDE // 2
    sign1 = sign_of(rising1)
    targets = []
    for h in range(2):
        target = iota((1, LANES), 1).astype(F32) + float(h * LANES)
        targets.append(jnp.where(rising1, float(TOPK - 1) - target, target))
    local = [jnp.zeros((SUB, LANES), F32) for _ in range(2)]
    for i in range(slots // LANES):
        rows = slice(i * LANES, (i + 1) * LANES)
        place = jnp.sum(seen[rows, :], axis=1, keepdims=True)
        for h in range(2):
            chosen = jnp.where(place == targets[h], column[rows, :], 0.0)
            local[h] += jnp.sum(chosen.reshape(LANES // SUB, SUB, LANES), axis=0)
    for h in range(2):
        list1[0, h:h + 1, :] = jnp.sum(local[h], axis=0, keepdims=True) * sign1
    merged = gathered[...]
    total = merged[0:ENT] + merged[ENT:2 * ENT] + merged[2 * ENT:3 * ENT]
    for b in range(SIDE):
        cand1[b] = total[:, b * LANES:(b + 1) * LANES]

    pl.semaphore_wait(barrier, SIDE - 1 + half - 1)

    def to(src, dst, ssem, rsem, device):
        return pltpu.make_async_remote_copy(
            src_ref=src, dst_ref=dst, send_sem=ssem, recv_sem=rsem,
            device_id={"scen": device}, device_id_type=MESH,
        )

    first = [to(list1.at[0], got1.at[x], send1, recv1, o * half + yc) for o in across]
    cfirst = [to(cand1.at[o], cgot1.at[x], csend1, crecv1, o * half + yc) for o in across]
    for copy in first:
        copy.start()
    for copy in cfirst:
        copy.start()
    got1[x] = list1[0]
    cgot1[x] = cand1[x]

    def settle(slots_of, others, sem):
        every = slots_of.at[pl.ds(0, others)]
        pltpu.make_async_copy(every, every, sem).wait()

    settle(got1, SIDE - 1, recv1)
    slot = iota((1, LANES), 1)
    all1 = got1[...]
    lists = jnp.concatenate([lists_down(all1[:, h, :]) for h in range(2)], axis=0)
    rising2 = yc >= half // 2
    lists = merge(lists, sign_of((slot & 4) != 0), 4, sign_of((slot & 2) != 0))
    lists = merge(lists, sign_of((slot & 2) != 0), 2, sign_of((slot & 1) != 0))
    lists = merge(lists, sign_of((slot & 1) != 0), 1, sign_of(rising2))
    for h in range(2):
        list2[0, h:h + 1, :] = along_lanes(lists[h * LANES:(h + 1) * LANES])
    second = [to(list2.at[0], got2.at[yc], send2, recv2, x * half + o) for o in along]
    for copy in second:
        copy.start()
    got2[yc] = list2[0]

    settle(cgot1, SIDE - 1, crecv1)
    cand2[0] = jnp.sum(cgot1[...], axis=0)
    csecond = [to(cand2.at[0], cgot2.at[yc], csend2, crecv2, x * half + o) for o in along]
    for copy in csecond:
        copy.start()
    cgot2[yc] = cand2[0]

    settle(got2, half - 1, recv2)
    all2 = got2[...]
    lists = jnp.concatenate([lists_down(all2[:, h, :]) for h in range(2)], axis=0)
    lists = merge(lists, sign_of((slot & 8) != 0), 8, sign_of((slot & 4) != 0))
    lists = merge(lists, sign_of((slot & 4) != 0), 4, sign_of((slot & 2) != 0))
    lists = merge(lists, sign_of((slot & 2) != 0), 2, sign_of((slot & 1) != 0))
    lists = merge(lists, sign_of((slot & 1) != 0), 1, F32(1.0))
    for h in range(2):
        tail_out[h:h + 1, :] = along_lanes(lists[h * LANES:(h + 1) * LANES])

    settle(cgot2, half - 1, crecv2)
    summed = jnp.sum(cgot2[...], axis=0)
    flipped[...] = jnp.concatenate([summed] * (LANES // ENT), axis=0).T
    cand_out[...] = flipped[pl.ds(pl.multiple_of(yc * SUB, SUB), SUB), 0:ENT]

    settle(got1, SIDE - 1, send1)
    settle(cgot1, SIDE - 1, csend1)
    settle(got2, half - 1, send2)
    settle(cgot2, half - 1, csend2)


def body(shocks, factor_sens, notional, moneyness, desk_entity, scenario_counts, candidate_ids):
    slots, factors = shocks.shape
    instruments = factor_sens.shape[1]
    half = SIDE * CORES
    hbm = pl.BlockSpec(memory_space=pltpu.HBM)
    vmem = pl.BlockSpec(memory_space=pltpu.VMEM)
    dma = pltpu.SemaphoreType.DMA
    tail, cand = pl.pallas_call(
        kernel,
        out_shape=(
            pltpu.VMEM((2, LANES), F32),
            pltpu.VMEM((SUB, ENT), F32),
        ),
        in_specs=[pl.BlockSpec(memory_space=pltpu.SMEM)] + [hbm] * 6,
        out_specs=(vmem, vmem),
        scratch_shapes=[
            pltpu.VMEM((slots, factors), BF16),
            pltpu.VMEM((factors, instruments), BF16),
            pltpu.VMEM((SUB, LANES), F32),
            pltpu.VMEM((SUB, LANES), F32),
            pltpu.VMEM((1, K), jnp.int32),
            pltpu.VMEM((SUB, LANES), jnp.int32),
            pltpu.VMEM((TILE, instruments // 2), F32),
            pltpu.VMEM((SUB, LANES), F32),
            pltpu.VMEM((slots, PIECES * LANES), BF16),
            pltpu.VMEM((PIECES * LANES, TILE), BF16),
            pltpu.VMEM((slots, LANES), F32),
            pltpu.VMEM((slots // LANES, SUB, LANES), F32),
            pltpu.VMEM((slots, LANES), F32),
            pltpu.VMEM((3 * ENT, SIDE * LANES), F32),
            pltpu.VMEM((1, 2, LANES), F32),
            pltpu.VMEM((1, 2, LANES), F32),
            pltpu.VMEM((SIDE, 2, LANES), F32),
            pltpu.VMEM((half, 2, LANES), F32),
            pltpu.VMEM((SIDE, ENT, LANES), F32),
            pltpu.VMEM((1, ENT, LANES), F32),
            pltpu.VMEM((SIDE, ENT, LANES), F32),
            pltpu.VMEM((half, ENT, LANES), F32),
            pltpu.VMEM((LANES, LANES), F32),
            dma((4 + slots // TILE,)),
            dma((4,)),
            dma, dma, dma, dma, dma, dma, dma, dma,
        ],
        compiler_params=pltpu.CompilerParams(
            collective_id=0, has_side_effects=True, vmem_limit_bytes=48 * 1024 * 1024
        ),
        name="tail_search",
    )(
        scenario_counts,
        *[
            pltpu.with_memory_space_constraint(array, pltpu.HBM)
            for array in (
                shocks,
                factor_sens,
                notional.reshape(SUB, LANES),
                moneyness.reshape(SUB, LANES),
                desk_entity.reshape(1, K),
                candidate_ids.reshape(SUB, LANES),
            )
        ],
    )
    return tail.reshape(TOPK), cand


def solution(mesh):
    both = ("grp", "scen")
    return jax.shard_map(
        body,
        mesh=mesh,
        in_specs=(P(both, None), P(), P(), P(), P(), P(both), P("grp")),
        out_specs=(P("grp"), P(both, None)),
        check_vma=False,
    )
```

```python
import functools

import jax
import jax.numpy as jnp
from jax import lax
from jax.experimental import pallas as pl
from jax.experimental.pallas import tpu as pltpu
from jax.sharding import PartitionSpec as P

K = 64
INSTR = 16
ENT = 8
TOPK = 256
SIDE = 8
CORES = 2
LANES = 128
SUB = 8
TILE = 256
STRIP = 32
PIECES = 3
FIRST = 4
FAR_SIDE = (4, 3, 5, 2, 6, 1, 7)
FAR_HALF = (8, 9, 7, 6, 10, 5, 11, 4, 12, 3, 13, 2, 14, 1, 15)
FLOOR = -1e30
MESH = pl.DeviceIdType.MESH
F32 = jnp.float32
BF16 = jnp.bfloat16


def iota(shape, dim):
    return lax.broadcasted_iota(jnp.int32, shape, dim)


def pieces(array, count):
    out = []
    for _ in range(count):
        part = array.astype(BF16).astype(F32)
        out.append(part)
        array = array - part
    return out


def pair_sum(left, right, step):
    low = (iota(left.shape, 1) & step) == 0
    up = left + pltpu.roll(left, LANES - step, 1)
    down = right + pltpu.roll(right, step, 1)
    return jnp.where(low, up, down)


def merge(stored, own, step, after):
    value = stored * own
    x = jnp.maximum(value, pltpu.roll(value, step, 1)) * after
    for stride in (128, 64, 32, 16, 8):
        y = x.reshape(TOPK // (2 * stride), 2, stride, LANES)
        a, b = y[:, 0], y[:, 1]
        x = jnp.stack([jnp.maximum(a, b), jnp.minimum(a, b)], axis=1).reshape(TOPK, LANES)
    y = x.reshape(TOPK // SUB, SUB, LANES)
    at = iota(y.shape, 1)
    for stride in (4, 2, 1):
        low = (at & stride) == 0
        if stride == 4:
            other = pltpu.roll(y, 4, 1)
        else:
            other = jnp.where(low, pltpu.roll(y, SUB - stride, 1), pltpu.roll(y, stride, 1))
        y = jnp.where(low, jnp.maximum(y, other), jnp.minimum(y, other))
    return y.reshape(TOPK, LANES)


def lists_down(rows):
    copies = LANES // rows.shape[0]
    return jnp.concatenate([rows] * copies, axis=0).T


def along_lanes(column):
    same = iota(column.shape, 0) == iota(column.shape, 1)
    return jnp.sum(jnp.where(same, column, 0.0), axis=0, keepdims=True)


def sign_of(bit):
    return jnp.where(bit, F32(-1.0), F32(1.0))


def search(
    units, cv, shocks, sens, notional, moneyness, desk_entity, ids,
    tail_out, cand_out,
    sh, fs, nv, mv, dv, iv, base_soft, terms, indicator, column, spread, seen, by_entity, split,
    list1, list2, got1, got2, cand1, cand2, cgot1, cgot2, flipped,
    load_sem, small_sem, send1, recv1, send2, recv2, csend1, crecv1, csend2, crecv2,
):
    slots, factors = sh.shape
    turns = slots // TILE
    wide = sens.shape[1] // 2
    deep = factors // FIRST
    me = lax.axis_index("scen")
    x, yc = me // (SIDE * CORES), me % (SIDE * CORES)
    half = SIDE * CORES
    across = [lax.rem(x + d, SIDE) for d in FAR_SIDE]
    along = [lax.rem(yc + d, half) for d in FAR_HALF]

    def copy_in(src, dst, n):
        return pltpu.make_async_copy(src, dst, load_sem.at[n])

    def part(ref, r0, rn, c0, cn):
        return ref.at[pl.ds(r0, rn), pl.ds(c0, cn)]

    def load(n, r=None):
        if n == "rows":
            rows = pl.ds(r * TILE, TILE)
            return copy_in(shocks.at[rows], sh.at[rows], 2 * FIRST + r)
        if n == "right":
            return copy_in(part(sens, 0, factors, wide, wide), part(fs, 0, factors, wide, wide), 2 * FIRST)
        at = n % FIRST * deep
        if n < FIRST:
            where = (0, TILE, at, deep)
            return copy_in(part(shocks, *where), part(sh, *where), n)
        where = (at, deep, 0, wide)
        return copy_in(part(sens, *where), part(fs, *where), n)

    small = [
        pltpu.make_async_copy(src, dst, small_sem.at[n])
        for n, (src, dst) in enumerate(
            [(moneyness, mv), (notional, nv), (desk_entity, dv), (ids, iv)]
        )
    ]
    for n in range(FIRST):
        load(n).start()
        load(FIRST + n).start()
    for copy in small:
        copy.start()
    for r in range(1, turns):
        load("rows", r).start()
    load("right").start()

    barrier = pltpu.get_barrier_semaphore()
    for other in across:
        pl.semaphore_signal(barrier, inc=1, device_id={"scen": other * half + yc}, device_id_type=MESH)
    for other in along:
        pl.semaphore_signal(barrier, inc=1, device_id={"scen": x * half + other}, device_id_type=MESH)

    for copy in small:
        copy.wait()

    lane = iota((LANES, LANES), 0)
    desk = 8 * (4 * ((lane // 2) % 2) + 2 * ((lane // 4) % 2) + (lane // 8) % 2) + lane // 16
    entity = jnp.concatenate([dv[...], jnp.full((1, LANES - K), -1, jnp.int32)], axis=1).astype(F32)
    entity = jnp.sum(jnp.where(desk == iota((LANES, LANES), 1), entity, 0.0), axis=1, keepdims=True)
    target = iota((LANES, TILE), 1)
    hit = (entity == target.astype(F32)) | (target >= LANES)
    owner = jnp.where(hit, -1.0, 0.0).astype(BF16)
    for p in range(PIECES):
        indicator[p * LANES:(p + 1) * LANES, :] = owner
    indicator[PIECES * LANES:, :] = jnp.zeros((LANES, TILE), BF16)
    terms[:, PIECES * LANES:] = jnp.zeros((slots, LANES), BF16)
    money = mv[...]
    base_soft[...] = jnp.maximum(money, 0.0) + jnp.log(1.0 + jnp.exp(-jnp.abs(money)))
    base = me * slots
    count = cv[0]

    free = [[0, 1], [0, 1]]
    for array in jax.tree.leaves(units):
        pltpu.matmul_pop(array)

    def push(m, tile):
        register = free[m].pop(0)
        pltpu.matmul_push_rhs(tile, register, m)
        return register

    def multiply(m, total, left, register):
        pltpu.matmul_acc_lhs(total, left, register)
        if register is not None:
            free[m].append(register)

    depth = factors // TILE
    tiles = [(c, r * TILE, TILE) for c in range(2) for r in range(turns)]
    order = [(k, t) for k in range(len(tiles)) for t in range(depth)]
    staged = []

    def stage(n):
        if n < len(order):
            k, t = order[n]
            c = tiles[k][0]
            staged.append([
                push(m, fs[t * TILE:(t + 1) * TILE, (2 * c + m) * TILE:(2 * c + m + 1) * TILE])
                for m in range(2)
            ])

    def step(n, hold):
        k, t = order[n]
        _, first, height = tiles[k]
        if not hold:
            stage(n + 1)
        registers = staged.pop(0)
        for q in range(0, height, STRIP):
            left = sh[first + q:first + q + STRIP, t * TILE:(t + 1) * TILE]
            for m in range(2):
                multiply(m, units[m]["value"][k % 2][q // STRIP], left, registers[m] if q == 0 else None)
        if hold and k == 0 and t == depth - 1:
            stage(n + 1)

    def price(k, s):
        c, first, _ = tiles[k]
        quads = []
        for m in range(2):
            found = pltpu.matmul_pop(units[m]["value"][k % 2][s // STRIP])
            for h in range(2):
                b = 4 * c + 2 * m + h
                v = found[:, h * LANES:(h + 1) * LANES] + mv[b:b + 1, :]
                soft = jnp.maximum(v, 0.0) + jnp.log(1.0 + jnp.exp(-jnp.abs(v)))
                quads.append(nv[b:b + 1, :] * (soft - base_soft[b:b + 1, :]))
        sums = pair_sum(pair_sum(quads[0], quads[1], 8), pair_sum(quads[2], quads[3], 8), 4)
        rows = slice(first + s, first + s + STRIP)
        if c == 0:
            column[rows, :] = sums
        else:
            sums = pair_sum(column[rows, :], sums, 2)
            for p, term in enumerate(pieces(sums, PIECES)):
                terms[rows, p * LANES:(p + 1) * LANES] = term.astype(BF16)

    def total_loss(r):
        for t in range(2):
            for m in range(2):
                at = r * TILE + m * LANES
                register = push(m, indicator[t * TILE:(t + 1) * TILE, :])
                multiply(m, units[m]["sums"], terms[at:at + LANES, t * TILE:(t + 1) * TILE], register)

    def spread_loss(r):
        for m in range(2):
            i = 2 * r + m
            total = pltpu.matmul_pop(units[m]["sums"])
            loss = jnp.where(i * LANES + iota((LANES, LANES), 0) < count, total[:, LANES:], FLOOR)
            column[i * LANES:(i + 1) * LANES, :] = loss
            spread[i] = loss.T[0:SUB]
            by_entity[i] = total[:, :LANES].T[0:ENT]

    def split_sums(r):
        found = pieces(jnp.concatenate([by_entity[2 * r], by_entity[2 * r + 1]], axis=1), 3)
        split[...] = jnp.concatenate(found + [jnp.zeros((ENT, TILE), F32)], axis=0).astype(BF16)

    def gather(r, t):
        here = base + r * TILE + iota((TILE, LANES), 0)
        for m in range(2):
            b = 4 * m + 2 * t
            wanted = jnp.concatenate(
                [jnp.where(iv[b + h:b + h + 1, :] == here, 1.0, 0.0).astype(BF16) for h in range(2)], axis=1
            )
            register = push(m, wanted)
            multiply(m, units[m]["gather"][t], split[...], register)

    def compare(i, b):
        mine = column[i * LANES:(i + 1) * LANES, :].reshape(LANES // SUB, SUB, LANES)
        theirs = spread[b][None]
        if i < b:
            ahead = mine >= theirs
        elif i > b:
            ahead = mine > theirs
        else:
            at = iota(mine.shape, 0) * SUB + iota(mine.shape, 1)
            ahead = (mine > theirs) | ((mine == theirs) & (at < iota(mine.shape, 2)))
        seen[b] += jnp.sum(jnp.where(ahead, 1.0, 0.0), axis=0)

    def rank(blocks):
        old = range(blocks[0])
        for b in old:
            for i in blocks:
                compare(i, b)
        for b in blocks:
            for i in (*old, *blocks):
                compare(i, b)

    def chunk(k, **work):
        @pl.when(me >= 0)
        def _():
            for t in range(depth):
                if k == 0 and t % 2 == 0:
                    load(t // 2).wait()
                    load(FIRST + t // 2).wait()
                    stage(t)
                if k == turns - 1 and t == depth - 1:
                    load("right").wait()
                step(k * depth + t, k == 0 and t % 2 == 1)
                if k > 0:
                    price(k - 1, t * STRIP)
                for piece in work.get("at%d" % t, ()):
                    piece()

    pairs = [(2 * r, 2 * r + 1) for r in range(turns)]
    seen[...] = jnp.zeros(seen.shape, F32)
    chunk(0)
    for k in range(1, turns):
        load("rows", k).wait()
        chunk(k)
    chunk(turns)
    chunk(turns + 1)
    chunk(turns + 2, at1=[lambda: total_loss(0)], at4=[lambda: spread_loss(0)], at5=[lambda: split_sums(0)])
    chunk(
        turns + 3,
        at1=[lambda: total_loss(1)],
        at2=[lambda: gather(0, 0)],
        at3=[lambda: gather(0, 1)],
        at4=[lambda: spread_loss(1), lambda: rank(pairs[0])],
        at5=[lambda: split_sums(1)],
    )
    total_loss(2)
    for t in range(depth):
        price(2 * turns - 1, t * STRIP)
    spread_loss(2)
    gather(1, 0)
    gather(1, 1)
    total_loss(3)
    rank(pairs[1])
    rank(pairs[2])
    spread_loss(3)
    rank(pairs[3])

    rising1 = x >= SIDE // 2
    sign1 = sign_of(rising1)
    target = iota((TOPK, LANES), 0).astype(F32)
    target = jnp.where(rising1, float(TOPK - 1) - target, target)
    chosen = jnp.zeros((TOPK, LANES), F32)
    for b in range(slots // LANES):
        place = jnp.sum(seen[b], axis=0, keepdims=True)
        chosen += jnp.where(place == target, spread[b][0:1], 0.0)
    ordered = jnp.broadcast_to(jnp.sum(chosen, axis=1, keepdims=True) * sign1, (TOPK, LANES))
    for h in range(2):
        list1[0, h:h + 1, :] = along_lanes(ordered[h * LANES:(h + 1) * LANES])

    pl.semaphore_wait(barrier, SIDE - 1 + half - 1)

    def to(src, dst, ssem, rsem, device):
        return pltpu.make_async_remote_copy(
            src_ref=src, dst_ref=dst, send_sem=ssem, recv_sem=rsem,
            device_id={"scen": device}, device_id_type=MESH,
        )

    first = [to(list1.at[0], got1.at[x], send1, recv1, o * half + yc) for o in across]
    cfirst = [to(cand1.at[o], cgot1.at[x], csend1, crecv1, o * half + yc) for o in across]
    for copy in first:
        copy.start()
    got1[x] = list1[0]
    for r in (2, 3):
        split_sums(r)
        gather(r, 0)
        gather(r, 1)
    for m in range(2):
        for t in range(2):
            found = pltpu.matmul_pop(units[m]["gather"][t])
            found = found[0:ENT] + found[ENT:2 * ENT] + found[2 * ENT:3 * ENT]
            for h in range(2):
                cand1[4 * m + 2 * t + h] = found[:, h * LANES:(h + 1) * LANES]

    for copy in cfirst:
        copy.start()
    cgot1[x] = cand1[x]

    def settle(slots_of, others, sem):
        every = slots_of.at[pl.ds(0, others)]
        pltpu.make_async_copy(every, every, sem).wait()

    settle(got1, SIDE - 1, recv1)
    slot = iota((1, LANES), 1)
    all1 = got1[...]
    lists = jnp.concatenate([lists_down(all1[:, h, :]) for h in range(2)], axis=0)
    rising2 = yc >= half // 2
    lists = merge(lists, sign_of((slot & 4) != 0), 4, sign_of((slot & 2) != 0))
    lists = merge(lists, sign_of((slot & 2) != 0), 2, sign_of((slot & 1) != 0))
    lists = merge(lists, sign_of((slot & 1) != 0), 1, sign_of(rising2))
    for h in range(2):
        list2[0, h:h + 1, :] = along_lanes(lists[h * LANES:(h + 1) * LANES])
    second = [to(list2.at[0], got2.at[yc], send2, recv2, x * half + o) for o in along]
    for copy in second:
        copy.start()
    got2[yc] = list2[0]

    settle(cgot1, SIDE - 1, crecv1)
    cand2[0] = jnp.sum(cgot1[...], axis=0)
    csecond = [to(cand2.at[0], cgot2.at[yc], csend2, crecv2, x * half + o) for o in along]
    for copy in csecond:
        copy.start()
    cgot2[yc] = cand2[0]

    settle(got2, half - 1, recv2)
    all2 = got2[...]
    lists = jnp.concatenate([lists_down(all2[:, h, :]) for h in range(2)], axis=0)
    lists = merge(lists, sign_of((slot & 8) != 0), 8, sign_of((slot & 4) != 0))
    lists = merge(lists, sign_of((slot & 4) != 0), 4, sign_of((slot & 2) != 0))
    lists = merge(lists, sign_of((slot & 2) != 0), 2, sign_of((slot & 1) != 0))
    settle(cgot2, half - 1, crecv2)
    summed = jnp.sum(cgot2[...], axis=0)
    flipped[...] = jnp.concatenate([summed] * (LANES // ENT), axis=0).T
    cand_out[...] = flipped[pl.ds(pl.multiple_of(yc * SUB, SUB), SUB), 0:ENT]
    lists = merge(lists, sign_of((slot & 1) != 0), 1, F32(1.0))
    for h in range(2):
        tail_out[h:h + 1, :] = along_lanes(lists[h * LANES:(h + 1) * LANES])

    settle(got1, SIDE - 1, send1)
    settle(cgot1, SIDE - 1, csend1)
    settle(got2, half - 1, send2)
    settle(cgot2, half - 1, csend2)


def kernel(*refs):
    units = []
    for m in range(2):
        total = pltpu.ACC(m)
        units.append({
            "value": [[total((STRIP, TILE), F32)] * (TILE // STRIP)] * 2,
            "sums": total((LANES, TILE), F32),
            "gather": [total((4 * ENT, TILE), F32)] * 2,
        })
    pl.run_scoped(lambda units: search(units, *refs), units)


def body(shocks, factor_sens, notional, moneyness, desk_entity, scenario_counts, candidate_ids):
    slots, factors = shocks.shape
    instruments = factor_sens.shape[1]
    half = SIDE * CORES
    hbm = pl.BlockSpec(memory_space=pltpu.HBM)
    vmem = pl.BlockSpec(memory_space=pltpu.VMEM)
    dma = pltpu.SemaphoreType.DMA
    tail, cand = pl.pallas_call(
        kernel,
        out_shape=(
            pltpu.VMEM((2, LANES), F32),
            pltpu.VMEM((SUB, ENT), F32),
        ),
        in_specs=[pl.BlockSpec(memory_space=pltpu.SMEM)] + [hbm] * 6,
        out_specs=(vmem, vmem),
        scratch_shapes=[
            pltpu.VMEM((slots, factors), BF16),
            pltpu.VMEM((factors, instruments), BF16),
            pltpu.VMEM((SUB, LANES), F32),
            pltpu.VMEM((SUB, LANES), F32),
            pltpu.VMEM((1, K), jnp.int32),
            pltpu.VMEM((SUB, LANES), jnp.int32),
            pltpu.VMEM((SUB, LANES), F32),
            pltpu.VMEM((slots, 2 * TILE), BF16),
            pltpu.VMEM((2 * TILE, TILE), BF16),
            pltpu.VMEM((slots, LANES), F32),
            pltpu.VMEM((slots // LANES, SUB, LANES), F32),
            pltpu.VMEM((slots // LANES, SUB, LANES), F32),
            pltpu.VMEM((slots // LANES, ENT, LANES), F32),
            pltpu.VMEM((4 * ENT, TILE), BF16),
            pltpu.VMEM((1, 2, LANES), F32),
            pltpu.VMEM((1, 2, LANES), F32),
            pltpu.VMEM((SIDE, 2, LANES), F32),
            pltpu.VMEM((half, 2, LANES), F32),
            pltpu.VMEM((SIDE, ENT, LANES), F32),
            pltpu.VMEM((1, ENT, LANES), F32),
            pltpu.VMEM((SIDE, ENT, LANES), F32),
            pltpu.VMEM((half, ENT, LANES), F32),
            pltpu.VMEM((LANES, LANES), F32),
            dma((2 * FIRST + slots // TILE,)),
            dma((4,)),
            dma, dma, dma, dma, dma, dma, dma, dma,
        ],
        compiler_params=pltpu.CompilerParams(
            collective_id=0, has_side_effects=True, vmem_limit_bytes=48 * 1024 * 1024
        ),
        name="tail_search",
    )(
        scenario_counts,
        *[
            pltpu.with_memory_space_constraint(array, pltpu.HBM)
            for array in (
                shocks,
                factor_sens,
                notional.reshape(SUB, LANES),
                moneyness.reshape(SUB, LANES),
                desk_entity.reshape(1, K),
                candidate_ids.reshape(SUB, LANES),
            )
        ],
    )
    return tail.reshape(TOPK), cand


def solution(mesh):
    both = ("grp", "scen")
    return jax.shard_map(
        body,
        mesh=mesh,
        in_specs=(P(both, None), P(), P(), P(), P(), P(both), P("grp")),
        out_specs=(P("grp"), P(both, None)),
        check_vma=False,
    )
```

```python
import functools

import jax
import jax.numpy as jnp
from jax import lax
from jax.experimental import pallas as pl
from jax.experimental.pallas import tpu as pltpu
from jax.sharding import PartitionSpec as P

K = 64
INSTR = 16
ENT = 8
TOPK = 256
SIDE = 8
CORES = 2
LANES = 128
SUB = 8
TILE = 256
STRIP = 32
PIECES = 3
FIRST = 4
FAR_SIDE = (4, 3, 5, 2, 6, 1, 7)
FAR_HALF = (8, 9, 7, 6, 10, 5, 11, 4, 12, 3, 13, 2, 14, 1, 15)
FLOOR = -1e30
MESH = pl.DeviceIdType.MESH
F32 = jnp.float32
BF16 = jnp.bfloat16


def iota(shape, dim):
    return lax.broadcasted_iota(jnp.int32, shape, dim)


def pieces(array, count):
    out = []
    for _ in range(count):
        part = array.astype(BF16).astype(F32)
        out.append(part)
        array = array - part
    return out


def pair_sum(left, right, step):
    low = (iota(left.shape, 1) & step) == 0
    up = left + pltpu.roll(left, LANES - step, 1)
    down = right + pltpu.roll(right, step, 1)
    return jnp.where(low, up, down)


def merge(stored, own, step, after):
    value = stored * own
    x = jnp.maximum(value, pltpu.roll(value, step, 1)) * after
    for stride in (128, 64, 32, 16, 8):
        y = x.reshape(TOPK // (2 * stride), 2, stride, LANES)
        a, b = y[:, 0], y[:, 1]
        x = jnp.stack([jnp.maximum(a, b), jnp.minimum(a, b)], axis=1).reshape(TOPK, LANES)
    y = x.reshape(TOPK // SUB, SUB, LANES)
    at = iota(y.shape, 1)
    for stride in (4, 2, 1):
        low = (at & stride) == 0
        if stride == 4:
            other = pltpu.roll(y, 4, 1)
        else:
            other = jnp.where(low, pltpu.roll(y, SUB - stride, 1), pltpu.roll(y, stride, 1))
        y = jnp.where(low, jnp.maximum(y, other), jnp.minimum(y, other))
    return y.reshape(TOPK, LANES)


def lists_down(rows):
    copies = LANES // rows.shape[0]
    return jnp.concatenate([rows] * copies, axis=0).T


def along_lanes(column):
    same = iota(column.shape, 0) == iota(column.shape, 1)
    return jnp.sum(jnp.where(same, column, 0.0), axis=0, keepdims=True)


def sign_of(bit):
    return jnp.where(bit, F32(-1.0), F32(1.0))


def search(
    units, cv, shocks, sens, notional, moneyness, desk_entity, ids,
    tail_out, cand_out,
    sh, fs, nv, mv, dv, iv, base_soft, terms, indicator, column, spread, seen, by_entity, split,
    list1, list2, got1, got2, cand1, cand2, cgot1, cgot2, flipped,
    load_sem, small_sem, send1, recv1, send2, recv2, csend1, crecv1, csend2, crecv2,
):
    slots, factors = sh.shape
    turns = slots // TILE
    wide = sens.shape[1] // 2
    deep = factors // FIRST
    me = lax.axis_index("scen")
    x, yc = me // (SIDE * CORES), me % (SIDE * CORES)
    half = SIDE * CORES
    across = [lax.rem(x + d, SIDE) for d in FAR_SIDE]
    along = [lax.rem(yc + d, half) for d in FAR_HALF]

    def copy_in(src, dst, n):
        return pltpu.make_async_copy(src, dst, load_sem.at[n])

    def part(ref, r0, rn, c0, cn):
        return ref.at[pl.ds(r0, rn), pl.ds(c0, cn)]

    def load(n, r=None):
        if n == "rows":
            rows = pl.ds(r * TILE, TILE)
            return copy_in(shocks.at[rows], sh.at[rows], 2 * FIRST + r)
        if n == "right":
            where = (r * factors // 2, factors // 2, wide, wide)
            return copy_in(part(sens, *where), part(fs, *where), 2 * FIRST + (r and turns))
        at = n % FIRST * deep
        if n < FIRST:
            where = (0, TILE, at, deep)
            return copy_in(part(shocks, *where), part(sh, *where), n)
        where = (at, deep, 0, wide)
        return copy_in(part(sens, *where), part(fs, *where), n)

    small = [
        pltpu.make_async_copy(src, dst, small_sem.at[n])
        for n, (src, dst) in enumerate(
            [(moneyness, mv), (notional, nv), (desk_entity, dv), (ids, iv)]
        )
    ]
    def start_piece(n):
        load(n).start()
        load(FIRST + n).start()

    start_piece(0)
    for copy in small:
        copy.start()

    barrier = pltpu.get_barrier_semaphore()
    greeted = [other * half + yc for other in across] + [x * half + other for other in along]
    for n, other in enumerate(greeted):
        pl.semaphore_signal(barrier, inc=1, device_id={"scen": other}, device_id_type=MESH)
        if n == 4:
            start_piece(1)
        if n == 10:
            start_piece(2)
        if n == 16:
            start_piece(3)
    load("rows", 1).start()

    for copy in small:
        copy.wait()

    lane = iota((LANES, LANES), 0)
    desk = 8 * (4 * ((lane // 2) % 2) + 2 * ((lane // 4) % 2) + (lane // 8) % 2) + lane // 16
    entity = jnp.concatenate([dv[...], jnp.full((1, LANES - K), -1, jnp.int32)], axis=1).astype(F32)
    entity = jnp.sum(jnp.where(desk == iota((LANES, LANES), 1), entity, 0.0), axis=1, keepdims=True)
    target = iota((LANES, TILE), 1)
    hit = (entity == target.astype(F32)) | (target >= LANES)
    owner = jnp.where(hit, -1.0, 0.0).astype(BF16)
    for p in range(PIECES):
        indicator[p * LANES:(p + 1) * LANES, :] = owner
    indicator[PIECES * LANES:, :] = jnp.zeros((LANES, TILE), BF16)
    terms[:, PIECES * LANES:] = jnp.zeros((slots, LANES), BF16)
    money = mv[...]
    base_soft[...] = jnp.maximum(money, 0.0) + jnp.log(1.0 + jnp.exp(-jnp.abs(money)))
    base = me * slots
    count = cv[0]

    free = [[0, 1], [0, 1]]
    for array in jax.tree.leaves(units):
        pltpu.matmul_pop(array)

    def push(m, tile):
        register = free[m].pop(0)
        pltpu.matmul_push_rhs(tile, register, m)
        return register

    def multiply(m, total, left, register):
        pltpu.matmul_acc_lhs(total, left, register)
        if register is not None:
            free[m].append(register)

    depth = factors // TILE
    tiles = [(c, r * TILE, TILE) for c in range(2) for r in range(turns)]
    order = [(k, t) for k in range(len(tiles)) for t in range(depth)]
    staged = []

    def stage(n):
        if n < len(order):
            k, t = order[n]
            c = tiles[k][0]
            staged.append([
                push(m, fs[t * TILE:(t + 1) * TILE, (2 * c + m) * TILE:(2 * c + m + 1) * TILE])
                for m in range(2)
            ])

    def step(n, hold):
        k, t = order[n]
        _, first, height = tiles[k]
        if not hold:
            stage(n + 1)
        registers = staged.pop(0)
        for q in range(0, height, STRIP):
            left = sh[first + q:first + q + STRIP, t * TILE:(t + 1) * TILE]
            for m in range(2):
                multiply(m, units[m]["value"][k % 2][q // STRIP], left, registers[m] if q == 0 else None)
        if hold and k == 0 and t == depth - 1:
            stage(n + 1)

    def price(k, s):
        c, first, _ = tiles[k]
        quads = []
        for m in range(2):
            found = pltpu.matmul_pop(units[m]["value"][k % 2][s // STRIP])
            for h in range(2):
                b = 4 * c + 2 * m + h
                v = found[:, h * LANES:(h + 1) * LANES] + mv[b:b + 1, :]
                soft = jnp.maximum(v, 0.0) + jnp.log(1.0 + jnp.exp(-jnp.abs(v)))
                quads.append(nv[b:b + 1, :] * (soft - base_soft[b:b + 1, :]))
        sums = pair_sum(pair_sum(quads[0], quads[1], 8), pair_sum(quads[2], quads[3], 8), 4)
        rows = slice(first + s, first + s + STRIP)
        if c == 0:
            column[rows, :] = sums
        else:
            sums = pair_sum(column[rows, :], sums, 2)
            for p, term in enumerate(pieces(sums, PIECES)):
                terms[rows, p * LANES:(p + 1) * LANES] = term.astype(BF16)

    def total_loss(r):
        for t in range(2):
            for m in range(2):
                at = r * TILE + m * LANES
                register = push(m, indicator[t * TILE:(t + 1) * TILE, :])
                multiply(m, units[m]["sums"], terms[at:at + LANES, t * TILE:(t + 1) * TILE], register)

    def spread_loss(r):
        for m in range(2):
            i = 2 * r + m
            total = pltpu.matmul_pop(units[m]["sums"])
            loss = jnp.where(i * LANES + iota((LANES, LANES), 0) < count, total[:, LANES:], FLOOR)
            column[i * LANES:(i + 1) * LANES, :] = loss
            spread[i] = loss.T[0:SUB]
            by_entity[i] = total[:, :LANES].T[0:ENT]

    def split_sums(r):
        found = pieces(jnp.concatenate([by_entity[2 * r], by_entity[2 * r + 1]], axis=1), 3)
        split[...] = jnp.concatenate(found + [jnp.zeros((ENT, TILE), F32)], axis=0).astype(BF16)

    def gather(r, t):
        here = base + r * TILE + iota((TILE, LANES), 0)
        for m in range(2):
            b = 4 * m + 2 * t
            wanted = jnp.concatenate(
                [jnp.where(iv[b + h:b + h + 1, :] == here, 1.0, 0.0).astype(BF16) for h in range(2)], axis=1
            )
            register = push(m, wanted)
            multiply(m, units[m]["gather"][t], split[...], register)

    def compare(i, b):
        mine = column[i * LANES:(i + 1) * LANES, :].reshape(LANES // SUB, SUB, LANES)
        theirs = spread[b][None]
        if i < b:
            ahead = mine >= theirs
        elif i > b:
            ahead = mine > theirs
        else:
            at = iota(mine.shape, 0) * SUB + iota(mine.shape, 1)
            ahead = (mine > theirs) | ((mine == theirs) & (at < iota(mine.shape, 2)))
        seen[b] += jnp.sum(jnp.where(ahead, 1.0, 0.0), axis=0)

    def rank(blocks):
        old = range(blocks[0])
        for b in old:
            for i in blocks:
                compare(i, b)
        for b in blocks:
            for i in (*old, *blocks):
                compare(i, b)

    following = [[load("rows", 2)], [load("rows", 3)], [load("right", 0)], [load("right", 1)]]

    def chunk(k, **work):
        @pl.when(me >= 0)
        def _():
            for t in range(depth):
                if k == 0 and t % 2 == 0:
                    load(t // 2).wait()
                    load(FIRST + t // 2).wait()
                    for copy in following[t // 2]:
                        copy.start()
                    stage(t)
                if k == turns - 1 and t == depth - 1:
                    load("right", 0).wait()
                if k == turns and t == depth // 2 - 1:
                    load("right", 1).wait()
                step(k * depth + t, k == 0 and t % 2 == 1)
                if k > 0:
                    price(k - 1, t * STRIP)
                for piece in work.get("at%d" % t, ()):
                    piece()

    pairs = [(2 * r, 2 * r + 1) for r in range(turns)]
    seen[...] = jnp.zeros(seen.shape, F32)
    chunk(0)
    for k in range(1, turns):
        load("rows", k).wait()
        chunk(k)
    chunk(turns)
    chunk(turns + 1)
    chunk(turns + 2, at4=[lambda: total_loss(0)], at7=[lambda: spread_loss(0), lambda: split_sums(0)])
    chunk(
        turns + 3,
        at1=[lambda: rank(pairs[0])],
        at2=[lambda: gather(0, 0)],
        at3=[lambda: gather(0, 1)],
        at5=[lambda: total_loss(1)],
    )
    spread_loss(1)
    total_loss(2)
    for t in range(depth):
        price(2 * turns - 1, t * STRIP)
    spread_loss(2)
    total_loss(3)
    rank(pairs[1])
    rank(pairs[2])
    spread_loss(3)
    rank(pairs[3])

    rising1 = x >= SIDE // 2
    sign1 = sign_of(rising1)
    target = iota((TOPK, LANES), 0).astype(F32)
    target = jnp.where(rising1, float(TOPK - 1) - target, target)
    chosen = jnp.zeros((TOPK, LANES), F32)
    for b in range(slots // LANES):
        place = jnp.sum(seen[b], axis=0, keepdims=True)
        chosen += jnp.where(place == target, spread[b][0:1], 0.0)
    ordered = jnp.broadcast_to(jnp.sum(chosen, axis=1, keepdims=True) * sign1, (TOPK, LANES))
    for h in range(2):
        list1[0, h:h + 1, :] = along_lanes(ordered[h * LANES:(h + 1) * LANES])

    pl.semaphore_wait(barrier, SIDE - 1 + half - 1)

    def to(src, dst, ssem, rsem, device):
        return pltpu.make_async_remote_copy(
            src_ref=src, dst_ref=dst, send_sem=ssem, recv_sem=rsem,
            device_id={"scen": device}, device_id_type=MESH,
        )

    first = [to(list1.at[0], got1.at[x], send1, recv1, o * half + yc) for o in across]
    cfirst = [to(cand1.at[o], cgot1.at[x], csend1, crecv1, o * half + yc) for o in across]
    for copy in first:
        copy.start()
    got1[x] = list1[0]
    for r in range(1, turns):
        split_sums(r)
        gather(r, 0)
        gather(r, 1)
    for m in range(2):
        for t in range(2):
            found = pltpu.matmul_pop(units[m]["gather"][t])
            found = found[0:ENT] + found[ENT:2 * ENT] + found[2 * ENT:3 * ENT]
            for h in range(2):
                cand1[4 * m + 2 * t + h] = found[:, h * LANES:(h + 1) * LANES]

    for copy in cfirst:
        copy.start()
    cgot1[x] = cand1[x]

    def settle(slots_of, others, sem):
        every = slots_of.at[pl.ds(0, others)]
        pltpu.make_async_copy(every, every, sem).wait()

    settle(got1, SIDE - 1, recv1)
    slot = iota((1, LANES), 1)
    all1 = got1[...]
    lists = jnp.concatenate([lists_down(all1[:, h, :]) for h in range(2)], axis=0)
    rising2 = yc >= half // 2
    lists = merge(lists, sign_of((slot & 4) != 0), 4, sign_of((slot & 2) != 0))
    lists = merge(lists, sign_of((slot & 2) != 0), 2, sign_of((slot & 1) != 0))
    lists = merge(lists, sign_of((slot & 1) != 0), 1, sign_of(rising2))
    for h in range(2):
        list2[0, h:h + 1, :] = along_lanes(lists[h * LANES:(h + 1) * LANES])
    second = [to(list2.at[0], got2.at[yc], send2, recv2, x * half + o) for o in along]
    for copy in second:
        copy.start()
    got2[yc] = list2[0]

    settle(cgot1, SIDE - 1, crecv1)
    cand2[0] = jnp.sum(cgot1[...], axis=0)
    csecond = [to(cand2.at[0], cgot2.at[yc], csend2, crecv2, x * half + o) for o in along]
    for copy in csecond:
        copy.start()
    cgot2[yc] = cand2[0]

    settle(got2, half - 1, recv2)
    all2 = got2[...]
    lists = jnp.concatenate([lists_down(all2[:, h, :]) for h in range(2)], axis=0)
    lists = merge(lists, sign_of((slot & 8) != 0), 8, sign_of((slot & 4) != 0))
    lists = merge(lists, sign_of((slot & 4) != 0), 4, sign_of((slot & 2) != 0))
    lists = merge(lists, sign_of((slot & 2) != 0), 2, sign_of((slot & 1) != 0))
    settle(cgot2, half - 1, crecv2)
    summed = jnp.sum(cgot2[...], axis=0)
    flipped[...] = jnp.concatenate([summed] * (LANES // ENT), axis=0).T
    cand_out[...] = flipped[pl.ds(pl.multiple_of(yc * SUB, SUB), SUB), 0:ENT]
    lists = merge(lists, sign_of((slot & 1) != 0), 1, F32(1.0))
    for h in range(2):
        tail_out[h:h + 1, :] = along_lanes(lists[h * LANES:(h + 1) * LANES])

    settle(got1, SIDE - 1, send1)
    settle(cgot1, SIDE - 1, csend1)
    settle(got2, half - 1, send2)
    settle(cgot2, half - 1, csend2)


def kernel(*refs):
    units = []
    for m in range(2):
        total = pltpu.ACC(m)
        units.append({
            "value": [[total((STRIP, TILE), F32)] * (TILE // STRIP)] * 2,
            "sums": total((LANES, TILE), F32),
            "gather": [total((4 * ENT, TILE), F32)] * 2,
        })
    pl.run_scoped(lambda units: search(units, *refs), units)


def store(tail, cand, tail_out, cand_out, sems):
    copies = [
        pltpu.make_async_copy(tail, tail_out, sems.at[0]),
        pltpu.make_async_copy(cand, cand_out, sems.at[1]),
    ]
    for copy in copies:
        copy.start()
    for copy in copies:
        copy.wait()


def body(shocks, factor_sens, notional, moneyness, desk_entity, scenario_counts, candidate_ids):
    slots, factors = shocks.shape
    instruments = factor_sens.shape[1]
    half = SIDE * CORES
    hbm = pl.BlockSpec(memory_space=pltpu.HBM)
    vmem = pl.BlockSpec(memory_space=pltpu.VMEM)
    dma = pltpu.SemaphoreType.DMA
    tail, cand = pl.pallas_call(
        kernel,
        out_shape=(
            pltpu.VMEM((2, LANES), F32),
            pltpu.VMEM((SUB, ENT), F32),
        ),
        in_specs=[pl.BlockSpec(memory_space=pltpu.SMEM)] + [hbm] * 6,
        out_specs=(vmem, vmem),
        scratch_shapes=[
            pltpu.VMEM((slots, factors), BF16),
            pltpu.VMEM((factors, instruments), BF16),
            pltpu.VMEM((SUB, LANES), F32),
            pltpu.VMEM((SUB, LANES), F32),
            pltpu.VMEM((1, K), jnp.int32),
            pltpu.VMEM((SUB, LANES), jnp.int32),
            pltpu.VMEM((SUB, LANES), F32),
            pltpu.VMEM((slots, 2 * TILE), BF16),
            pltpu.VMEM((2 * TILE, TILE), BF16),
            pltpu.VMEM((slots, LANES), F32),
            pltpu.VMEM((slots // LANES, SUB, LANES), F32),
            pltpu.VMEM((slots // LANES, SUB, LANES), F32),
            pltpu.VMEM((slots // LANES, ENT, LANES), F32),
            pltpu.VMEM((4 * ENT, TILE), BF16),
            pltpu.VMEM((1, 2, LANES), F32),
            pltpu.VMEM((1, 2, LANES), F32),
            pltpu.VMEM((SIDE, 2, LANES), F32),
            pltpu.VMEM((half, 2, LANES), F32),
            pltpu.VMEM((SIDE, ENT, LANES), F32),
            pltpu.VMEM((1, ENT, LANES), F32),
            pltpu.VMEM((SIDE, ENT, LANES), F32),
            pltpu.VMEM((half, ENT, LANES), F32),
            pltpu.VMEM((LANES, LANES), F32),
            dma((2 * FIRST + slots // TILE + 1,)),
            dma((4,)),
            dma, dma, dma, dma, dma, dma, dma, dma,
        ],
        compiler_params=pltpu.CompilerParams(
            collective_id=0, has_side_effects=True, vmem_limit_bytes=48 * 1024 * 1024
        ),
        name="tail_search",
    )(
        scenario_counts,
        *[
            pltpu.with_memory_space_constraint(array, pltpu.HBM)
            for array in (
                shocks,
                factor_sens,
                notional.reshape(SUB, LANES),
                moneyness.reshape(SUB, LANES),
                desk_entity.reshape(1, K),
                candidate_ids.reshape(SUB, LANES),
            )
        ],
    )
    tail, cand = pl.pallas_call(
        store,
        out_shape=(pltpu.HBM((2, LANES), F32), pltpu.HBM((SUB, ENT), F32)),
        in_specs=[vmem, vmem],
        out_specs=(hbm, hbm),
        scratch_shapes=[dma((2,))],
        name="store",
    )(*[pltpu.with_memory_space_constraint(array, pltpu.VMEM) for array in (tail, cand)])
    return tail.reshape(TOPK), cand


def solution(mesh):
    both = ("grp", "scen")
    return jax.shard_map(
        body,
        mesh=mesh,
        in_specs=(P(both, None), P(), P(), P(), P(), P(both), P("grp")),
        out_specs=(P("grp"), P(both, None)),
        check_vma=False,
    )
```

```python
import functools

import jax
import jax.numpy as jnp
from jax import lax
from jax.experimental import pallas as pl
from jax.experimental.pallas import tpu as pltpu
from jax.sharding import PartitionSpec as P

K = 64
INSTR = 16
ENT = 8
TOPK = 256
SIDE = 8
CORES = 2
LANES = 128
SUB = 8
TILE = 256
STRIP = 32
PIECES = 3
FIRST = 4
FAR_SIDE = (4, 3, 5, 2, 6, 1, 7)
FAR_HALF = (8, 9, 7, 6, 10, 5, 11, 4, 12, 3, 13, 2, 14, 1, 15)
FLOOR = -1e30
MESH = pl.DeviceIdType.MESH
F32 = jnp.float32
BF16 = jnp.bfloat16


def iota(shape, dim):
    return lax.broadcasted_iota(jnp.int32, shape, dim)


def pieces(array, count):
    out = []
    for _ in range(count):
        part = array.astype(BF16).astype(F32)
        out.append(part)
        array = array - part
    return out


def pair_sum(left, right, step):
    low = (iota(left.shape, 1) & step) == 0
    up = left + pltpu.roll(left, LANES - step, 1)
    down = right + pltpu.roll(right, step, 1)
    return jnp.where(low, up, down)


def merge(stored, own, step, after):
    value = stored * own
    x = jnp.maximum(value, pltpu.roll(value, step, 1)) * after
    for stride in (128, 64, 32, 16, 8):
        y = x.reshape(TOPK // (2 * stride), 2, stride, LANES)
        a, b = y[:, 0], y[:, 1]
        x = jnp.stack([jnp.maximum(a, b), jnp.minimum(a, b)], axis=1).reshape(TOPK, LANES)
    y = x.reshape(TOPK // SUB, SUB, LANES)
    at = iota(y.shape, 1)
    for stride in (4, 2, 1):
        low = (at & stride) == 0
        later = pltpu.roll(y, SUB - stride, 1)
        earlier = later if stride == 4 else pltpu.roll(y, stride, 1)
        y = jnp.where(low, jnp.maximum(y, later), jnp.minimum(y, earlier))
    return y.reshape(TOPK, LANES)


def lists_down(rows):
    copies = LANES // rows.shape[0]
    return jnp.concatenate([rows] * copies, axis=0).T


def along_lanes(column):
    same = iota(column.shape, 0) == iota(column.shape, 1)
    return jnp.sum(jnp.where(same, column, 0.0), axis=0, keepdims=True)


def sign_of(bit):
    return jnp.where(bit, F32(-1.0), F32(1.0))


def search(
    units, cv, shocks, sens, notional, moneyness, desk_entity, ids,
    tail_out, cand_out,
    sh, fs, nv, mv, dv, iv, base_soft, terms, indicator, column, spread, seen, by_entity, split,
    list1, list2, got1, got2, cand1, cand2, cgot1, cgot2,
    load_sem, small_sem, send1, recv1, send2, recv2, csend1, crecv1, csend2, crecv2,
):
    slots, factors = sh.shape
    turns = slots // TILE
    wide = sens.shape[1] // 2
    deep = factors // FIRST
    me = lax.axis_index("scen")
    x, yc = me // (SIDE * CORES), me % (SIDE * CORES)
    half = SIDE * CORES
    across = [lax.rem(x + d, SIDE) for d in FAR_SIDE]
    along = [lax.rem(yc + d, half) for d in FAR_HALF]

    def copy_in(src, dst, n):
        return pltpu.make_async_copy(src, dst, load_sem.at[n])

    def part(ref, r0, rn, c0, cn):
        return ref.at[pl.ds(r0, rn), pl.ds(c0, cn)]

    def load(n, r=None):
        if n == "rows":
            rows = pl.ds(r * TILE, TILE)
            return copy_in(shocks.at[rows], sh.at[rows], 2 * FIRST + r)
        if n == "right":
            where = (r * factors // 2, factors // 2, wide, wide)
            return copy_in(part(sens, *where), part(fs, *where), 2 * FIRST + (r and turns))
        at = n % FIRST * deep
        if n < FIRST:
            where = (0, TILE, at, deep)
            return copy_in(part(shocks, *where), part(sh, *where), n)
        where = (at, deep, 0, wide)
        return copy_in(part(sens, *where), part(fs, *where), n)

    small = [
        pltpu.make_async_copy(src, dst, small_sem.at[n])
        for n, (src, dst) in enumerate(
            [(moneyness, mv), (notional, nv), (desk_entity, dv), (ids, iv)]
        )
    ]
    def start_piece(n):
        load(n).start()
        load(FIRST + n).start()

    start_piece(0)
    for copy in small:
        copy.start()

    barrier = pltpu.get_barrier_semaphore()
    greeted = [other * half + yc for other in across] + [x * half + other for other in along]
    for n, other in enumerate(greeted):
        pl.semaphore_signal(barrier, inc=1, device_id={"scen": other}, device_id_type=MESH)
        if n == 4:
            start_piece(1)
        if n == 10:
            start_piece(2)
        if n == 16:
            start_piece(3)
    load("rows", 1).start()

    for copy in small:
        copy.wait()

    lane = iota((LANES, LANES), 0)
    desk = 8 * (4 * ((lane // 2) % 2) + 2 * ((lane // 4) % 2) + (lane // 8) % 2) + lane // 16
    entity = jnp.concatenate([dv[...], jnp.full((1, LANES - K), -1, jnp.int32)], axis=1).astype(F32)
    entity = jnp.sum(jnp.where(desk == iota((LANES, LANES), 1), entity, 0.0), axis=1, keepdims=True)
    target = iota((LANES, TILE), 1)
    hit = (entity == target.astype(F32)) | (target >= LANES)
    owner = jnp.where(hit, -1.0, 0.0).astype(BF16)
    for p in range(PIECES):
        indicator[p * LANES:(p + 1) * LANES, :] = owner
    indicator[PIECES * LANES:, :] = jnp.zeros((LANES, TILE), BF16)
    terms[:, PIECES * LANES:] = jnp.zeros((slots, LANES), BF16)
    money = mv[...]
    base_soft[...] = jnp.maximum(money, 0.0) + jnp.log(1.0 + jnp.exp(-jnp.abs(money)))
    base = me * slots
    count = cv[0]

    free = [[0, 1], [0, 1]]
    for array in jax.tree.leaves(units):
        pltpu.matmul_pop(array)

    def push(m, tile):
        register = free[m].pop(0)
        pltpu.matmul_push_rhs(tile, register, m)
        return register

    def multiply(m, total, left, register):
        pltpu.matmul_acc_lhs(total, left, register)
        if register is not None:
            free[m].append(register)

    depth = factors // TILE
    tiles = [(c, r * TILE, TILE) for c in range(2) for r in range(turns)]
    order = [(k, t) for k in range(len(tiles)) for t in range(depth)]
    staged = []

    def stage(n):
        if n < len(order):
            k, t = order[n]
            c = tiles[k][0]
            staged.append([
                push(m, fs[t * TILE:(t + 1) * TILE, (2 * c + m) * TILE:(2 * c + m + 1) * TILE])
                for m in range(2)
            ])

    def step(n, hold):
        k, t = order[n]
        _, first, height = tiles[k]
        if not hold:
            stage(n + 1)
        registers = staged.pop(0)
        for q in range(0, height, STRIP):
            left = sh[first + q:first + q + STRIP, t * TILE:(t + 1) * TILE]
            for m in range(2):
                multiply(m, units[m]["value"][k % 2][q // STRIP], left, registers[m] if q == 0 else None)
        if hold and k == 0 and t == depth - 1:
            stage(n + 1)

    def price(k, s):
        c, first, _ = tiles[k]
        quads = []
        for m in range(2):
            found = pltpu.matmul_pop(units[m]["value"][k % 2][s // STRIP])
            for h in range(2):
                b = 4 * c + 2 * m + h
                v = found[:, h * LANES:(h + 1) * LANES] + mv[b:b + 1, :]
                soft = jnp.maximum(v, 0.0) + jnp.log(1.0 + jnp.exp(-jnp.abs(v)))
                quads.append(nv[b:b + 1, :] * (soft - base_soft[b:b + 1, :]))
        sums = pair_sum(pair_sum(quads[0], quads[1], 8), pair_sum(quads[2], quads[3], 8), 4)
        rows = slice(first + s, first + s + STRIP)
        if c == 0:
            column[rows, :] = sums
        else:
            sums = pair_sum(column[rows, :], sums, 2)
            for p, term in enumerate(pieces(sums, PIECES)):
                terms[rows, p * LANES:(p + 1) * LANES] = term.astype(BF16)

    def total_loss(r):
        for t in range(2):
            for m in range(2):
                at = r * TILE + m * LANES
                register = push(m, indicator[t * TILE:(t + 1) * TILE, :])
                multiply(m, units[m]["sums"], terms[at:at + LANES, t * TILE:(t + 1) * TILE], register)

    def spread_loss(r):
        for m in range(2):
            i = 2 * r + m
            total = pltpu.matmul_pop(units[m]["sums"])
            loss = jnp.where(i * LANES + iota((LANES, LANES), 0) < count, total[:, LANES:], FLOOR)
            column[i * LANES:(i + 1) * LANES, :] = loss
            spread[i] = loss.T[0:SUB]
            by_entity[i] = total[:, :LANES].T[0:ENT]

    def split_sums(r):
        found = pieces(jnp.concatenate([by_entity[2 * r], by_entity[2 * r + 1]], axis=1), 3)
        split[...] = jnp.concatenate(found + [jnp.zeros((ENT, TILE), F32)], axis=0).astype(BF16)

    def gather(r, t):
        here = base + r * TILE + iota((TILE, LANES), 0)
        for m in range(2):
            b = 4 * m + 2 * t
            wanted = jnp.concatenate(
                [jnp.where(iv[b + h:b + h + 1, :] == here, 1.0, 0.0).astype(BF16) for h in range(2)], axis=1
            )
            register = push(m, wanted)
            multiply(m, units[m]["gather"][t], split[...], register)

    def compare(i, b):
        mine = column[i * LANES:(i + 1) * LANES, :].reshape(LANES // SUB, SUB, LANES)
        theirs = spread[b][None]
        if i < b:
            ahead = mine >= theirs
        elif i > b:
            ahead = mine > theirs
        else:
            at = iota(mine.shape, 0) * SUB + iota(mine.shape, 1)
            ahead = (mine > theirs) | ((mine == theirs) & (at < iota(mine.shape, 2)))
        seen[b] += jnp.sum(jnp.where(ahead, 1.0, 0.0), axis=0)

    def rank(blocks):
        old = range(blocks[0])
        for b in old:
            for i in blocks:
                compare(i, b)
        for b in blocks:
            for i in (*old, *blocks):
                compare(i, b)

    following = [[load("rows", 2)], [load("rows", 3)], [load("right", 0)], [load("right", 1)]]

    def chunk(k, **work):
        @pl.when(me >= 0)
        def _():
            for t in range(depth):
                if k == 0 and t % 2 == 0:
                    load(t // 2).wait()
                    load(FIRST + t // 2).wait()
                    for copy in following[t // 2]:
                        copy.start()
                    stage(t)
                if k == turns - 1 and t == depth - 1:
                    load("right", 0).wait()
                if k == turns and t == depth // 2 - 1:
                    load("right", 1).wait()
                step(k * depth + t, k == 0 and t % 2 == 1)
                if k > 0:
                    price(k - 1, t * STRIP)
                for piece in work.get("at%d" % t, ()):
                    piece()

    pairs = [(2 * r, 2 * r + 1) for r in range(turns)]
    seen[...] = jnp.zeros(seen.shape, F32)
    chunk(0)
    for k in range(1, turns):
        load("rows", k).wait()
        chunk(k)
    chunk(turns)
    chunk(turns + 1)
    chunk(turns + 2, at4=[lambda: total_loss(0)], at7=[lambda: spread_loss(0)])
    chunk(
        turns + 3,
        at1=[lambda: rank(pairs[0])],
        at3=[lambda: total_loss(1)],
        at6=[lambda: spread_loss(1)],
    )
    total_loss(2)
    for t in range(depth):
        price(2 * turns - 1, t * STRIP)
    spread_loss(2)
    total_loss(3)
    rank(pairs[1])
    rank(pairs[2])
    spread_loss(3)
    rank(pairs[3])

    rising1 = x >= SIDE // 2
    sign1 = sign_of(rising1)
    target = iota((TOPK, LANES), 0).astype(F32)
    target = jnp.where(rising1, float(TOPK - 1) - target, target)
    chosen = jnp.zeros((TOPK, LANES), F32)
    for b in range(slots // LANES):
        place = jnp.sum(seen[b], axis=0, keepdims=True)
        chosen += jnp.where(place == target, spread[b][0:1], 0.0)
    ordered = jnp.broadcast_to(jnp.sum(chosen, axis=1, keepdims=True) * sign1, (TOPK, LANES))
    for h in range(2):
        list1[0, h:h + 1, :] = along_lanes(ordered[h * LANES:(h + 1) * LANES])

    pl.semaphore_wait(barrier, SIDE - 1 + half - 1)

    def to(src, dst, ssem, rsem, device):
        return pltpu.make_async_remote_copy(
            src_ref=src, dst_ref=dst, send_sem=ssem, recv_sem=rsem,
            device_id={"scen": device}, device_id_type=MESH,
        )

    first = [to(list1.at[0], got1.at[x], send1, recv1, o * half + yc) for o in across]
    cfirst = [to(cand1.at[o], cgot1.at[x], csend1, crecv1, o * half + yc) for o in across]
    for copy in first:
        copy.start()
    got1[x] = list1[0]
    for r in range(turns):
        split_sums(r)
        gather(r, 0)
        gather(r, 1)
    for m in range(2):
        for t in range(2):
            found = pltpu.matmul_pop(units[m]["gather"][t])
            found = found[0:ENT] + found[ENT:2 * ENT] + found[2 * ENT:3 * ENT]
            for h in range(2):
                cand1[4 * m + 2 * t + h] = found[:, h * LANES:(h + 1) * LANES]

    for copy in cfirst:
        copy.start()
    cgot1[x] = cand1[x]

    def settle(slots_of, others, sem):
        every = slots_of.at[pl.ds(0, others)]
        pltpu.make_async_copy(every, every, sem).wait()

    settle(got1, SIDE - 1, recv1)
    slot = iota((1, LANES), 1)
    all1 = got1[...]
    lists = jnp.concatenate([lists_down(all1[:, h, :]) for h in range(2)], axis=0)
    rising2 = yc >= half // 2
    lists = merge(lists, sign_of((slot & 4) != 0), 4, sign_of((slot & 2) != 0))
    lists = merge(lists, sign_of((slot & 2) != 0), 2, sign_of((slot & 1) != 0))
    lists = merge(lists, sign_of((slot & 1) != 0), 1, sign_of(rising2))
    for h in range(2):
        list2[0, h:h + 1, :] = along_lanes(lists[h * LANES:(h + 1) * LANES])
    second = [to(list2.at[0], got2.at[yc], send2, recv2, x * half + o) for o in along]
    for copy in second:
        copy.start()
    got2[yc] = list2[0]

    settle(cgot1, SIDE - 1, crecv1)
    turned = jnp.concatenate([jnp.sum(cgot1[...], axis=0)] * (LANES // ENT), axis=0).T
    own_lanes = iota((SUB, LANES), 1) // ENT == iota((SUB, LANES), 0)
    for o in range(half):
        mine = jnp.where(own_lanes, turned[o * SUB:(o + 1) * SUB], 0.0)
        cand2[o] = jnp.sum(mine, axis=0, keepdims=True)
    csecond = [to(cand2.at[o], cgot2.at[yc], csend2, crecv2, x * half + o) for o in along]
    for copy in csecond:
        copy.start()
    cgot2[yc] = cand2[yc]

    settle(got2, half - 1, recv2)
    all2 = got2[...]
    lists = jnp.concatenate([lists_down(all2[:, h, :]) for h in range(2)], axis=0)
    lists = merge(lists, sign_of((slot & 8) != 0), 8, sign_of((slot & 4) != 0))
    lists = merge(lists, sign_of((slot & 4) != 0), 4, sign_of((slot & 2) != 0))
    lists = merge(lists, sign_of((slot & 2) != 0), 2, sign_of((slot & 1) != 0))
    settle(cgot2, half - 1, crecv2)
    summed = jnp.broadcast_to(jnp.sum(cgot2[...], axis=0), (SUB, LANES))
    by_row = summed
    for q in range(1, SUB):
        by_row = jnp.where(iota((SUB, LANES), 0) == q, pltpu.roll(summed, LANES - q * ENT, 1), by_row)
    cand_out[...] = by_row[:, 0:ENT]
    lists = merge(lists, sign_of((slot & 1) != 0), 1, F32(1.0))
    for h in range(2):
        tail_out[h:h + 1, :] = along_lanes(lists[h * LANES:(h + 1) * LANES])

    settle(got1, SIDE - 1, send1)
    settle(cgot1, SIDE - 1, csend1)
    settle(got2, half - 1, send2)
    settle(cgot2, half - 1, csend2)


def kernel(*refs):
    units = []
    for m in range(2):
        total = pltpu.ACC(m)
        units.append({
            "value": [[total((STRIP, TILE), F32)] * (TILE // STRIP)] * 2,
            "sums": total((LANES, TILE), F32),
            "gather": [total((4 * ENT, TILE), F32)] * 2,
        })
    pl.run_scoped(lambda units: search(units, *refs), units)


def store(tail, cand, tail_out, cand_out, sems):
    copies = [
        pltpu.make_async_copy(tail, tail_out, sems.at[0]),
        pltpu.make_async_copy(cand, cand_out, sems.at[1]),
    ]
    for copy in copies:
        copy.start()
    for copy in copies:
        copy.wait()


def body(shocks, factor_sens, notional, moneyness, desk_entity, scenario_counts, candidate_ids):
    slots, factors = shocks.shape
    instruments = factor_sens.shape[1]
    half = SIDE * CORES
    hbm = pl.BlockSpec(memory_space=pltpu.HBM)
    vmem = pl.BlockSpec(memory_space=pltpu.VMEM)
    dma = pltpu.SemaphoreType.DMA
    tail, cand = pl.pallas_call(
        kernel,
        out_shape=(
            pltpu.VMEM((2, LANES), F32),
            pltpu.VMEM((SUB, ENT), F32),
        ),
        in_specs=[pl.BlockSpec(memory_space=pltpu.SMEM)] + [hbm] * 6,
        out_specs=(vmem, vmem),
        scratch_shapes=[
            pltpu.VMEM((slots, factors), BF16),
            pltpu.VMEM((factors, instruments), BF16),
            pltpu.VMEM((SUB, LANES), F32),
            pltpu.VMEM((SUB, LANES), F32),
            pltpu.VMEM((1, K), jnp.int32),
            pltpu.VMEM((SUB, LANES), jnp.int32),
            pltpu.VMEM((SUB, LANES), F32),
            pltpu.VMEM((slots, 2 * TILE), BF16),
            pltpu.VMEM((2 * TILE, TILE), BF16),
            pltpu.VMEM((slots, LANES), F32),
            pltpu.VMEM((slots // LANES, SUB, LANES), F32),
            pltpu.VMEM((slots // LANES, SUB, LANES), F32),
            pltpu.VMEM((slots // LANES, ENT, LANES), F32),
            pltpu.VMEM((4 * ENT, TILE), BF16),
            pltpu.VMEM((1, 2, LANES), F32),
            pltpu.VMEM((1, 2, LANES), F32),
            pltpu.VMEM((SIDE, 2, LANES), F32),
            pltpu.VMEM((half, 2, LANES), F32),
            pltpu.VMEM((SIDE, ENT, LANES), F32),
            pltpu.VMEM((half, 1, LANES), F32),
            pltpu.VMEM((SIDE, ENT, LANES), F32),
            pltpu.VMEM((half, 1, LANES), F32),
            dma((2 * FIRST + slots // TILE + 1,)),
            dma((4,)),
            dma, dma, dma, dma, dma, dma, dma, dma,
        ],
        compiler_params=pltpu.CompilerParams(
            collective_id=0, has_side_effects=True, vmem_limit_bytes=48 * 1024 * 1024
        ),
        name="tail_search",
    )(
        scenario_counts,
        *[
            pltpu.with_memory_space_constraint(array, pltpu.HBM)
            for array in (
                shocks,
                factor_sens,
                notional.reshape(SUB, LANES),
                moneyness.reshape(SUB, LANES),
                desk_entity.reshape(1, K),
                candidate_ids.reshape(SUB, LANES),
            )
        ],
    )
    tail, cand = pl.pallas_call(
        store,
        out_shape=(pltpu.HBM((2, LANES), F32), pltpu.HBM((SUB, ENT), F32)),
        in_specs=[vmem, vmem],
        out_specs=(hbm, hbm),
        scratch_shapes=[dma((2,))],
        name="store",
    )(*[pltpu.with_memory_space_constraint(array, pltpu.VMEM) for array in (tail, cand)])
    return tail.reshape(TOPK), cand


def solution(mesh):
    both = ("grp", "scen")
    return jax.shard_map(
        body,
        mesh=mesh,
        in_specs=(P(both, None), P(), P(), P(), P(), P(both), P("grp")),
        out_specs=(P("grp"), P(both, None)),
        check_vma=False,
    )
```

```python
import functools

import jax
import jax.numpy as jnp
from jax import lax
from jax.experimental import pallas as pl
from jax.experimental.pallas import tpu as pltpu
from jax.sharding import PartitionSpec as P

K = 64
INSTR = 16
ENT = 8
TOPK = 256
SIDE = 8
CORES = 2
LANES = 128
SUB = 8
TILE = 256
STRIP = 32
PIECES = 3
FIRST = 4
FAR_SIDE = (4, 3, 5, 2, 6, 1, 7)
FAR_HALF = (8, 9, 7, 6, 10, 5, 11, 4, 12, 3, 13, 2, 14, 1, 15)
FLOOR = -1e30
MESH = pl.DeviceIdType.MESH
F32 = jnp.float32
BF16 = jnp.bfloat16


def iota(shape, dim):
    return lax.broadcasted_iota(jnp.int32, shape, dim)


def pieces(array, count):
    out = []
    for _ in range(count):
        part = array.astype(BF16).astype(F32)
        out.append(part)
        array = array - part
    return out


def pair_sum(left, right, step):
    low = (iota(left.shape, 1) & step) == 0
    up = left + pltpu.roll(left, LANES - step, 1)
    down = right + pltpu.roll(right, step, 1)
    return jnp.where(low, up, down)


def merge(stored, own, step, after, met=None):
    value = stored * own
    other = pltpu.roll(value, step, 1) if met is None else -(met * own)
    x = jnp.maximum(value, other) * after
    for stride in (128, 64, 32, 16, 8):
        y = x.reshape(TOPK // (2 * stride), 2, stride, LANES)
        a, b = y[:, 0], y[:, 1]
        x = jnp.stack([jnp.maximum(a, b), jnp.minimum(a, b)], axis=1).reshape(TOPK, LANES)
    y = x.reshape(TOPK // SUB, SUB, LANES)
    at = iota(y.shape, 1)
    for stride in (4, 2, 1):
        low = (at & stride) == 0
        later = pltpu.roll(y, SUB - stride, 1)
        earlier = later if stride == 4 else pltpu.roll(y, stride, 1)
        y = jnp.where(low, jnp.maximum(y, later), jnp.minimum(y, earlier))
    return y.reshape(TOPK, LANES)


def lists_down(rows):
    copies = LANES // rows.shape[0]
    return jnp.concatenate([rows] * copies, axis=0).T


def halves_swapped(rows):
    middle = rows.shape[0] // 2
    return jnp.concatenate([rows[middle:], rows[:middle]], axis=0)


def along_lanes(column):
    same = iota(column.shape, 0) == iota(column.shape, 1)
    return jnp.sum(jnp.where(same, column, 0.0), axis=0, keepdims=True)


def sign_of(bit):
    return jnp.where(bit, F32(-1.0), F32(1.0))


def search(
    units, cv, shocks, sens, notional, moneyness, desk_entity, ids,
    tail_out, cand_out,
    sh, fs, nv, mv, dv, iv, base_soft, terms, indicator, column, spread, seen, by_entity, split,
    list1, list2, got1, got2, cand1, cand2, cgot1, cgot2,
    load_sem, small_sem, send1, recv1, send2, recv2, csend1, crecv1, csend2, crecv2,
):
    slots, factors = sh.shape
    turns = slots // TILE
    wide = sens.shape[1] // 2
    deep = factors // FIRST
    me = lax.axis_index("scen")
    x, yc = me // (SIDE * CORES), me % (SIDE * CORES)
    half = SIDE * CORES
    across = [lax.rem(x + d, SIDE) for d in FAR_SIDE]
    along = [lax.rem(yc + d, half) for d in FAR_HALF]

    def copy_in(src, dst, n):
        return pltpu.make_async_copy(src, dst, load_sem.at[n])

    def part(ref, r0, rn, c0, cn):
        return ref.at[pl.ds(r0, rn), pl.ds(c0, cn)]

    def load(n, r=None):
        if n == "rows":
            rows = pl.ds(r * TILE, TILE)
            return copy_in(shocks.at[rows], sh.at[rows], 2 * FIRST + r)
        if n == "right":
            where = (r * factors // 2, factors // 2, wide, wide)
            return copy_in(part(sens, *where), part(fs, *where), 2 * FIRST + (r and turns))
        at = n % FIRST * deep
        if n < FIRST:
            where = (0, TILE, at, deep)
            return copy_in(part(shocks, *where), part(sh, *where), n)
        where = (at, deep, 0, wide)
        return copy_in(part(sens, *where), part(fs, *where), n)

    small = [
        pltpu.make_async_copy(src, dst, small_sem.at[n])
        for n, (src, dst) in enumerate(
            [(moneyness, mv), (notional, nv), (desk_entity, dv), (ids, iv)]
        )
    ]
    def start_piece(n):
        load(n).start()
        load(FIRST + n).start()

    start_piece(0)
    for copy in small:
        copy.start()

    barrier = pltpu.get_barrier_semaphore()
    greeted = [other * half + yc for other in across] + [x * half + other for other in along]
    for n, other in enumerate(greeted):
        pl.semaphore_signal(barrier, inc=1, device_id={"scen": other}, device_id_type=MESH)
        if n == 4:
            start_piece(1)
        if n == 10:
            start_piece(2)
        if n == 16:
            start_piece(3)
    load("rows", 1).start()

    for copy in small:
        copy.wait()

    lane = iota((LANES, LANES), 0)
    desk = 8 * (4 * ((lane // 2) % 2) + 2 * ((lane // 4) % 2) + (lane // 8) % 2) + lane // 16
    entity = jnp.concatenate([dv[...], jnp.full((1, LANES - K), -1, jnp.int32)], axis=1).astype(F32)
    entity = jnp.sum(jnp.where(desk == iota((LANES, LANES), 1), entity, 0.0), axis=1, keepdims=True)
    target = iota((LANES, TILE), 1)
    hit = (entity == target.astype(F32)) | (target >= LANES)
    owner = jnp.where(hit, -1.0, 0.0).astype(BF16)
    for p in range(PIECES):
        indicator[p * LANES:(p + 1) * LANES, :] = owner
    indicator[PIECES * LANES:, :] = jnp.zeros((LANES, TILE), BF16)
    terms[:, PIECES * LANES:] = jnp.zeros((slots, LANES), BF16)
    money = mv[...]
    base_soft[...] = jnp.maximum(money, 0.0) + jnp.log(1.0 + jnp.exp(-jnp.abs(money)))
    base = me * slots
    count = cv[0]

    free = [[0, 1], [0, 1]]
    for array in jax.tree.leaves(units):
        pltpu.matmul_pop(array)

    def push(m, tile):
        register = free[m].pop(0)
        pltpu.matmul_push_rhs(tile, register, m)
        return register

    def multiply(m, total, left, register):
        pltpu.matmul_acc_lhs(total, left, register)
        if register is not None:
            free[m].append(register)

    depth = factors // TILE
    tiles = [(c, r * TILE, TILE) for c in range(2) for r in range(turns)]
    order = [(k, t) for k in range(len(tiles)) for t in range(depth)]
    staged = []

    def stage(n):
        if n < len(order):
            k, t = order[n]
            c = tiles[k][0]
            staged.append([
                push(m, fs[t * TILE:(t + 1) * TILE, (2 * c + m) * TILE:(2 * c + m + 1) * TILE])
                for m in range(2)
            ])

    def step(n, hold):
        k, t = order[n]
        _, first, height = tiles[k]
        if not hold:
            stage(n + 1)
        registers = staged.pop(0)
        for q in range(0, height, STRIP):
            left = sh[first + q:first + q + STRIP, t * TILE:(t + 1) * TILE]
            for m in range(2):
                multiply(m, units[m]["value"][k % 2][q // STRIP], left, registers[m] if q == 0 else None)
        if hold and k == 0 and t == depth - 1:
            stage(n + 1)

    def price(k, s):
        c, first, _ = tiles[k]
        quads = []
        for m in range(2):
            found = pltpu.matmul_pop(units[m]["value"][k % 2][s // STRIP])
            for h in range(2):
                b = 4 * c + 2 * m + h
                v = found[:, h * LANES:(h + 1) * LANES] + mv[b:b + 1, :]
                soft = jnp.maximum(v, 0.0) + jnp.log(1.0 + jnp.exp(-jnp.abs(v)))
                quads.append(nv[b:b + 1, :] * (soft - base_soft[b:b + 1, :]))
        sums = pair_sum(pair_sum(quads[0], quads[1], 8), pair_sum(quads[2], quads[3], 8), 4)
        rows = slice(first + s, first + s + STRIP)
        if c == 0:
            column[rows, :] = sums
        else:
            sums = pair_sum(column[rows, :], sums, 2)
            for p, term in enumerate(pieces(sums, PIECES)):
                terms[rows, p * LANES:(p + 1) * LANES] = term.astype(BF16)

    def total_loss(r):
        for t in range(2):
            for m in range(2):
                at = r * TILE + m * LANES
                register = push(m, indicator[t * TILE:(t + 1) * TILE, :])
                multiply(m, units[m]["sums"], terms[at:at + LANES, t * TILE:(t + 1) * TILE], register)

    def spread_loss(r):
        for m in range(2):
            i = 2 * r + m
            total = pltpu.matmul_pop(units[m]["sums"])
            loss = jnp.where(i * LANES + iota((LANES, LANES), 0) < count, total[:, LANES:], FLOOR)
            column[i * LANES:(i + 1) * LANES, :] = loss
            spread[i] = loss.T[0:SUB]
            by_entity[i] = total[:, :LANES].T[0:ENT]

    def split_sums(r):
        found = pieces(jnp.concatenate([by_entity[2 * r], by_entity[2 * r + 1]], axis=1), 3)
        split[...] = jnp.concatenate(found + [jnp.zeros((ENT, TILE), F32)], axis=0).astype(BF16)

    def gather(r, t):
        here = base + r * TILE + iota((TILE, LANES), 0)
        for m in range(2):
            b = 4 * m + 2 * t
            wanted = jnp.concatenate(
                [jnp.where(iv[b + h:b + h + 1, :] == here, 1.0, 0.0).astype(BF16) for h in range(2)], axis=1
            )
            register = push(m, wanted)
            multiply(m, units[m]["gather"][t], split[...], register)

    def compare(i, b):
        mine = column[i * LANES:(i + 1) * LANES, :].reshape(LANES // SUB, SUB, LANES)
        theirs = spread[b][None]
        if i < b:
            ahead = mine >= theirs
        elif i > b:
            ahead = mine > theirs
        else:
            at = iota(mine.shape, 0) * SUB + iota(mine.shape, 1)
            ahead = (mine > theirs) | ((mine == theirs) & (at < iota(mine.shape, 2)))
        seen[b] += jnp.sum(jnp.where(ahead, 1.0, 0.0), axis=0)

    def rank(blocks):
        old = range(blocks[0])
        for b in old:
            for i in blocks:
                compare(i, b)
        for b in blocks:
            for i in (*old, *blocks):
                compare(i, b)

    following = [[load("rows", 2)], [load("rows", 3)], [load("right", 0)], [load("right", 1)]]

    def chunk(k, **work):
        @pl.when(me >= 0)
        def _():
            for t in range(depth):
                if k == 0 and t % 2 == 0:
                    load(t // 2).wait()
                    load(FIRST + t // 2).wait()
                    for copy in following[t // 2]:
                        copy.start()
                    stage(t)
                if k == turns - 1 and t == depth - 1:
                    load("right", 0).wait()
                if k == turns and t == depth // 2 - 1:
                    load("right", 1).wait()
                step(k * depth + t, k == 0 and t % 2 == 1)
                if k > 0:
                    price(k - 1, t * STRIP)
                for piece in work.get("at%d" % t, ()):
                    piece()

    pairs = [(2 * r, 2 * r + 1) for r in range(turns)]
    seen[...] = jnp.zeros(seen.shape, F32)
    chunk(0)
    for k in range(1, turns):
        load("rows", k).wait()
        chunk(k)
    chunk(turns)
    chunk(turns + 1)
    chunk(turns + 2, at4=[lambda: total_loss(0)], at7=[lambda: spread_loss(0)])
    chunk(
        turns + 3,
        at1=[lambda: rank(pairs[0])],
        at3=[lambda: total_loss(1)],
        at6=[lambda: spread_loss(1)],
    )
    total_loss(2)
    for t in range(depth):
        price(2 * turns - 1, t * STRIP)
    spread_loss(2)
    total_loss(3)
    rank(pairs[1])
    rank(pairs[2])
    spread_loss(3)
    rank(pairs[3])

    rising1 = x >= SIDE // 2
    sign1 = sign_of(rising1)
    target = iota((TOPK, LANES), 0).astype(F32)
    target = jnp.where(rising1, float(TOPK - 1) - target, target)
    chosen = jnp.zeros((TOPK, LANES), F32)
    for b in range(slots // LANES):
        place = jnp.sum(seen[b], axis=0, keepdims=True)
        chosen += jnp.where(place == target, spread[b][0:1], 0.0)
    ordered = jnp.broadcast_to(jnp.sum(chosen, axis=1, keepdims=True) * sign1, (TOPK, LANES))
    for h in range(2):
        list1[0, h:h + 1, :] = along_lanes(ordered[h * LANES:(h + 1) * LANES])

    pl.semaphore_wait(barrier, SIDE - 1 + half - 1)

    def to(src, dst, ssem, rsem, device):
        return pltpu.make_async_remote_copy(
            src_ref=src, dst_ref=dst, send_sem=ssem, recv_sem=rsem,
            device_id={"scen": device}, device_id_type=MESH,
        )

    first = [to(list1.at[0], got1.at[x], send1, recv1, o * half + yc) for o in across]
    cfirst = [to(cand1.at[o], cgot1.at[x], csend1, crecv1, o * half + yc) for o in across]
    for copy in first:
        copy.start()
    got1[x] = list1[0]
    for r in range(turns):
        split_sums(r)
        gather(r, 0)
        gather(r, 1)
    for m in range(2):
        for t in range(2):
            found = pltpu.matmul_pop(units[m]["gather"][t])
            found = found[0:ENT] + found[ENT:2 * ENT] + found[2 * ENT:3 * ENT]
            for h in range(2):
                cand1[4 * m + 2 * t + h] = found[:, h * LANES:(h + 1) * LANES]

    for copy in cfirst:
        copy.start()
    cgot1[x] = cand1[x]

    def settle(slots_of, others, sem):
        every = slots_of.at[pl.ds(0, others)]
        pltpu.make_async_copy(every, every, sem).wait()

    settle(got1, SIDE - 1, recv1)
    slot = iota((1, LANES), 1)
    all1 = got1[...]
    lists = jnp.concatenate([lists_down(all1[:, h, :]) for h in range(2)], axis=0)
    met = jnp.concatenate([lists_down(halves_swapped(all1[:, h, :])) for h in range(2)], axis=0)
    rising2 = yc >= half // 2
    lists = merge(lists, sign_of((slot & 4) != 0), 4, sign_of((slot & 2) != 0), met)
    lists = merge(lists, sign_of((slot & 2) != 0), 2, sign_of((slot & 1) != 0))
    lists = merge(lists, sign_of((slot & 1) != 0), 1, sign_of(rising2))
    for h in range(2):
        list2[0, h:h + 1, :] = along_lanes(lists[h * LANES:(h + 1) * LANES])
    second = [to(list2.at[0], got2.at[yc], send2, recv2, x * half + o) for o in along]
    for copy in second:
        copy.start()
    got2[yc] = list2[0]

    settle(cgot1, SIDE - 1, crecv1)
    turned = jnp.concatenate([jnp.sum(cgot1[...], axis=0)] * (LANES // ENT), axis=0).T
    own_lanes = iota((SUB, LANES), 1) // ENT == iota((SUB, LANES), 0)
    for o in range(half):
        mine = jnp.where(own_lanes, turned[o * SUB:(o + 1) * SUB], 0.0)
        cand2[o] = jnp.sum(mine, axis=0, keepdims=True)
    csecond = [to(cand2.at[o], cgot2.at[yc], csend2, crecv2, x * half + o) for o in along]
    for copy in csecond:
        copy.start()
    cgot2[yc] = cand2[yc]

    settle(got2, half - 1, recv2)
    all2 = got2[...]
    lists = jnp.concatenate([lists_down(all2[:, h, :]) for h in range(2)], axis=0)
    met = jnp.concatenate([lists_down(halves_swapped(all2[:, h, :])) for h in range(2)], axis=0)
    lists = merge(lists, sign_of((slot & 8) != 0), 8, sign_of((slot & 4) != 0), met)
    lists = merge(lists, sign_of((slot & 4) != 0), 4, sign_of((slot & 2) != 0))
    lists = merge(lists, sign_of((slot & 2) != 0), 2, sign_of((slot & 1) != 0))
    settle(cgot2, half - 1, crecv2)
    summed = jnp.broadcast_to(jnp.sum(cgot2[...], axis=0), (SUB, LANES))
    by_row = summed
    for q in range(1, SUB):
        by_row = jnp.where(iota((SUB, LANES), 0) == q, pltpu.roll(summed, LANES - q * ENT, 1), by_row)
    cand_out[...] = by_row[:, 0:ENT]
    lists = merge(lists, sign_of((slot & 1) != 0), 1, F32(1.0))
    for h in range(2):
        tail_out[h:h + 1, :] = along_lanes(lists[h * LANES:(h + 1) * LANES])

    settle(got1, SIDE - 1, send1)
    settle(cgot1, SIDE - 1, csend1)
    settle(got2, half - 1, send2)
    settle(cgot2, half - 1, csend2)


def kernel(*refs):
    units = []
    for m in range(2):
        total = pltpu.ACC(m)
        units.append({
            "value": [[total((STRIP, TILE), F32)] * (TILE // STRIP)] * 2,
            "sums": total((LANES, TILE), F32),
            "gather": [total((4 * ENT, TILE), F32)] * 2,
        })
    pl.run_scoped(lambda units: search(units, *refs), units)


def store(tail, cand, tail_out, cand_out, sems):
    copies = [
        pltpu.make_async_copy(tail, tail_out, sems.at[0]),
        pltpu.make_async_copy(cand, cand_out, sems.at[1]),
    ]
    for copy in copies:
        copy.start()
    for copy in copies:
        copy.wait()


def body(shocks, factor_sens, notional, moneyness, desk_entity, scenario_counts, candidate_ids):
    slots, factors = shocks.shape
    instruments = factor_sens.shape[1]
    half = SIDE * CORES
    hbm = pl.BlockSpec(memory_space=pltpu.HBM)
    vmem = pl.BlockSpec(memory_space=pltpu.VMEM)
    dma = pltpu.SemaphoreType.DMA
    tail, cand = pl.pallas_call(
        kernel,
        out_shape=(
            pltpu.VMEM((2, LANES), F32),
            pltpu.VMEM((SUB, ENT), F32),
        ),
        in_specs=[pl.BlockSpec(memory_space=pltpu.SMEM)] + [hbm] * 6,
        out_specs=(vmem, vmem),
        scratch_shapes=[
            pltpu.VMEM((slots, factors), BF16),
            pltpu.VMEM((factors, instruments), BF16),
            pltpu.VMEM((SUB, LANES), F32),
            pltpu.VMEM((SUB, LANES), F32),
            pltpu.VMEM((1, K), jnp.int32),
            pltpu.VMEM((SUB, LANES), jnp.int32),
            pltpu.VMEM((SUB, LANES), F32),
            pltpu.VMEM((slots, 2 * TILE), BF16),
            pltpu.VMEM((2 * TILE, TILE), BF16),
            pltpu.VMEM((slots, LANES), F32),
            pltpu.VMEM((slots // LANES, SUB, LANES), F32),
            pltpu.VMEM((slots // LANES, SUB, LANES), F32),
            pltpu.VMEM((slots // LANES, ENT, LANES), F32),
            pltpu.VMEM((4 * ENT, TILE), BF16),
            pltpu.VMEM((1, 2, LANES), F32),
            pltpu.VMEM((1, 2, LANES), F32),
            pltpu.VMEM((SIDE, 2, LANES), F32),
            pltpu.VMEM((half, 2, LANES), F32),
            pltpu.VMEM((SIDE, ENT, LANES), F32),
            pltpu.VMEM((half, 1, LANES), F32),
            pltpu.VMEM((SIDE, ENT, LANES), F32),
            pltpu.VMEM((half, 1, LANES), F32),
            dma((2 * FIRST + slots // TILE + 1,)),
            dma((4,)),
            dma, dma, dma, dma, dma, dma, dma, dma,
        ],
        compiler_params=pltpu.CompilerParams(
            collective_id=0, has_side_effects=True, vmem_limit_bytes=48 * 1024 * 1024
        ),
        name="tail_search",
    )(
        scenario_counts,
        *[
            pltpu.with_memory_space_constraint(array, pltpu.HBM)
            for array in (
                shocks,
                factor_sens,
                notional.reshape(SUB, LANES),
                moneyness.reshape(SUB, LANES),
                desk_entity.reshape(1, K),
                candidate_ids.reshape(SUB, LANES),
            )
        ],
    )
    tail, cand = pl.pallas_call(
        store,
        out_shape=(pltpu.HBM((2, LANES), F32), pltpu.HBM((SUB, ENT), F32)),
        in_specs=[vmem, vmem],
        out_specs=(hbm, hbm),
        scratch_shapes=[dma((2,))],
        name="store",
    )(*[pltpu.with_memory_space_constraint(array, pltpu.VMEM) for array in (tail, cand)])
    return tail.reshape(TOPK), cand


def solution(mesh):
    both = ("grp", "scen")
    return jax.shard_map(
        body,
        mesh=mesh,
        in_specs=(P(both, None), P(), P(), P(), P(), P(both), P("grp")),
        out_specs=(P("grp"), P(both, None)),
        check_vma=False,
    )
```
